256 devices in a mesh: groups: 2 (over z), steps: 128 (over y, x, core).
Axes of the slice: x: 8, y: 8, z: 2, core: 2. Of those that a mesh axis runs over, the one named last changes fastest.
The devices are a block of a 8x8x16 slice.
Arguments:
- states: float32 [256, 4, 4096], P(('groups', 'steps')), parts along dimension 0, may hold values from -6 to 6
- t_sched: int32 [514], P('groups'), parts along dimension 0, may hold values from 0 to 999, as said below
- advances: int32 [4], P('groups'), parts along dimension 0, may hold values from 1 to 128, as said below
- in_weight: bfloat16 [320, 4], replicated, may hold values from -3 to 3
- time_weight: float32 [320, 320], replicated, may hold values from -0.3125 to 0.3125
- mid_weight: bfloat16 [320, 320], replicated, may hold values from -0.3125 to 0.3125
- out_weight: bfloat16 [4, 320], replicated, may hold values from -0.3125 to 0.3125
Outputs:
- final_states: float32 [256, 4, 4096], P(('groups', 'steps')), parts along dimension 0
- errors: float32 [4, 4, 128], P('groups', None, 'steps'), parts along dimension 0
The draws below stay inside these ranges and needn't reach their ends.
There are 2 independent parts, one for each index of `groups`. The reference program is written for one: setup_inputs(seed, part) draws one part's arguments, and reference() takes and returns one part's arrays. A program takes and returns all parts, laid end to end along the dimension named above; an argument that names none is the same for every part. Nothing has to cross between parts.
Inputs may be any that keep to these rules, and one draw needn't show every extreme that they name: `t_sched`: strictly decreasing. Some round advances by exactly 128.
All inputs are finite; a program needn't handle non-finite values.
Results may differ from the reference program's by a relative error of at most 0.0024.
Values sent between devices are 32-bit elements; how exact they have to be, the bound alone decides.
No kernel may reach another device: no remote copies, remote signals or barrier semaphores. Data moves between devices by JAX's collectives and lax.ppermute only.
A program may use at most 64 MiB of HBM per device.

```python
import math
import jax
import jax.numpy as jnp
from jax import lax

CH = 320
LAT = 4
TSTEPS = 1000
ROWS = 4096
ITERS = 4
ROUNDS = 2
WINDOW = 128
SCHED = 257
ADV_MOST = 128


def draw_t_sched(key, part):
    picked = jax.random.permutation(key, TSTEPS)[:SCHED].astype(jnp.int32)
    return -jnp.sort(-picked)


def draw_advances(key, part):
    first_key = jax.random.fold_in(key, 11)
    second_key = jax.random.fold_in(key, 12)
    values = jax.random.randint(first_key, (ROUNDS,), 1, ADV_MOST + 1).astype(jnp.int32)
    chosen = jax.random.randint(second_key, (), 0, ROUNDS)
    return jnp.where(jnp.arange(ROUNDS) == chosen, ADV_MOST, values).astype(jnp.int32)


def block_levels(key, dims, shards, low, high):
    loudness = 1.0
    for position, blocks in shards:
        draws = jax.random.uniform(jax.random.fold_in(jax.random.fold_in(key, 6), position), (blocks,), jnp.float32, low / len(shards), high / len(shards))
        loudness = loudness * jnp.repeat(jnp.exp(draws), dims[position] // blocks).reshape((-1,) + (1,) * (len(dims) - 1 - position))
    return loudness


def gaussian(stream_key, shape, width, limit, cuts=(), kind=jnp.bfloat16):
    entries = jax.random.normal(stream_key, shape, jnp.float32) * width
    if len(cuts) > 0:
        entries = block_levels(stream_key, shape, cuts, -0.22, 0.18) * entries
    return jnp.clip(entries, min=-limit, max=limit).astype(kind)


def setup_inputs(seed: int = 0, part: int = 0) -> dict:
    streams_of = jax.random.split(jax.random.key(seed), 8)
    own_keys = jax.random.split(jax.random.fold_in(streams_of[7], part), 8)
    states = gaussian(own_keys[0], (WINDOW, LAT, ROWS), 1.0, 6.0, ((0, 128),), jnp.float32)
    t_sched = draw_t_sched(jax.random.fold_in(jax.random.fold_in(streams_of[7], part), 71), part)
    advances = draw_advances(jax.random.fold_in(jax.random.fold_in(streams_of[7], part), 71), part)
    in_weight = gaussian(streams_of[3], (CH, LAT), LAT ** -0.5, 3.0)
    time_weight = gaussian(streams_of[4], (CH, CH), CH ** -0.5, 0.3125, (), jnp.float32)
    mid_weight = gaussian(streams_of[5], (CH, CH), CH ** -0.5, 0.3125)
    out_weight = gaussian(streams_of[6], (LAT, CH), CH ** -0.5, 0.3125)
    return dict(states=states, t_sched=t_sched, advances=advances, in_weight=in_weight, time_weight=time_weight, mid_weight=mid_weight, out_weight=out_weight)


def alpha_table():
    levels = jnp.arange(TSTEPS, dtype=jnp.float32)
    low = math.sqrt(0.00085)
    high = math.sqrt(0.012)
    betas = (low + (high - low) * levels / (TSTEPS - 1)) ** 2
    return jnp.exp(jnp.cumsum(jnp.log1p(-betas)))

def time_features(stamp):
    halfwidth = CH // 2
    freqs = jnp.exp(-math.log(10000.0) * jnp.arange(halfwidth, dtype=jnp.float32) / halfwidth)
    angles = stamp.astype(jnp.float32) * freqs
    return jnp.concatenate([jnp.cos(angles), jnp.sin(angles)])

def denoise(state, embed, in_weight, mid_weight, out_weight):
    pre = jnp.dot(in_weight, state.astype(jnp.bfloat16), preferred_element_type=jnp.float32) + embed[:, None]
    hidden_one = jax.nn.silu(pre).astype(jnp.bfloat16)
    mixed = jnp.dot(mid_weight, hidden_one, preferred_element_type=jnp.float32)
    hidden_two = (jax.nn.silu(mixed) + pre).astype(jnp.bfloat16)
    return jnp.dot(out_weight, hidden_two, preferred_element_type=jnp.float32)

def reference(states, t_sched, advances, in_weight, time_weight, mid_weight, out_weight):
    alphas = alpha_table()
    window = states.shape[0]
    places = jnp.arange(window, dtype=jnp.int32)
    current = states
    window_start = jnp.int32(0)
    error_rows = []
    for round_no in range(ROUNDS):
        stamp_now = t_sched[window_start + places]
        stamp_next = t_sched[window_start + places + 1]
        alpha_now = alphas[stamp_now]
        alpha_next = alphas[stamp_next]
        coef_one = jnp.sqrt(alpha_next / alpha_now)
        coef_two = jnp.sqrt(1.0 - alpha_next) - coef_one * jnp.sqrt(1.0 - alpha_now)
        feats = jax.vmap(time_features)(stamp_now)
        embeds = jnp.dot(feats, time_weight.T, precision=lax.Precision.HIGHEST)
        sweep_rows = []
        for sweep in range(ITERS):
            noise = lax.map(lambda pair: denoise(pair[0], pair[1], in_weight, mid_weight, out_weight), (current, embeds))
            drift = (coef_one - 1.0)[:, None, None] * current + coef_two[:, None, None] * noise
            totals = jnp.cumsum(drift, axis=0)
            prefix = jnp.concatenate([jnp.zeros_like(drift[:1]), totals[:-1]], axis=0)
            updated = current[0:1] + prefix
            updated = jnp.concatenate([current[0:1], updated[1:]], axis=0)
            sweep_rows.append(lax.optimization_barrier(jnp.mean((updated - current) ** 2, axis=(1, 2))))
            current = updated
        error_rows.append(jnp.stack(sweep_rows))
        advance = advances[round_no]
        source = jnp.minimum(places + advance, window - 1).astype(jnp.int32)
        current = current[source]
        window_start = window_start + advance
    return (current, jnp.stack(error_rows))
```

```python
import functools
import math

import jax
import jax.numpy as jnp
import ml_dtypes
import numpy as np
from jax import lax
from jax.experimental import pallas as pl
from jax.experimental.pallas import tpu as pltpu
from jax.sharding import PartitionSpec as P

TSTEPS = 1000
ITERS = 4
ROUNDS = 2
RADIX = 32
LANES = 128
F32 = jnp.float32
BF16 = jnp.bfloat16


def three_parts(table):
    rest = np.asarray(table, np.float64)
    parts = []
    for _ in range(3):
        part = rest.astype(ml_dtypes.bfloat16)
        parts.append(part)
        rest = rest - part.astype(np.float64)
    return np.concatenate(parts, axis=1)


def tables(width):
    half = width // 2
    freqs = np.exp(-math.log(10000.0) * np.arange(half, dtype=np.float64) / half)
    digits = np.arange(RADIX, dtype=np.float64)
    coarse = freqs[:, None] * (digits * RADIX)[None]
    fine = freqs[:, None] * digits[None]
    levels = np.arange(RADIX * RADIX, dtype=np.float64)
    low, high = math.sqrt(0.00085), math.sqrt(0.012)
    betas = (low + (high - low) * levels / (TSTEPS - 1)) ** 2
    alphas = np.exp(np.cumsum(np.log1p(-betas)))
    root = np.sqrt(alphas).reshape(RADIX, RADIX).T
    rest = np.sqrt(1.0 - alphas).reshape(RADIX, RADIX).T
    table_a = np.concatenate([np.cos(coarse), np.sin(coarse), root, rest], axis=0)
    table_b = np.concatenate([np.cos(fine), np.sin(fine)], axis=0)
    return three_parts(table_a), three_parts(table_b)


def dot(left, right):
    return jnp.dot(left, right, preferred_element_type=F32)


def split2(value):
    high = value.astype(BF16)
    return high, (value - high.astype(F32)).astype(BF16)


def split3(value):
    high = value.astype(BF16)
    rest = value - high.astype(F32)
    mid = rest.astype(BF16)
    return high, mid, (rest - mid.astype(F32)).astype(BF16)


def one_hot(row, count):
    return (lax.broadcasted_iota(jnp.int32, (count, row.shape[1]), 0) == row).astype(F32)


def picard(
    group,
    adv_ref,
    stamps_ref,
    recv_ref,
    in_ref,
    time_ref,
    mid_ref,
    out_w_ref,
    table_a_ref,
    table_b_ref,
    send_ref,
    state,
    embed,
    bias,
    scale_x,
    scale_e,
    mid_half,
    left_in,
    left_out,
    squares,
):
    window, rows = recv_ref.shape
    channels, lat = in_ref.shape
    half = channels // 2
    depth = group * lat
    tiles = rows // depth
    iters = ROUNDS * ITERS

    stamps = stamps_ref[...]
    row = jnp.concatenate([stamps[k : k + 1] for k in (0, 2, 1, 3)], axis=1)
    hot_a = one_hot(row // RADIX, RADIX).astype(BF16)
    digit_b = row % RADIX
    hot_b = one_hot(digit_b, RADIX)
    hot_a3 = jnp.concatenate([hot_a] * 3, axis=0)
    now_b = hot_b[:, : 2 * window].astype(BF16)
    now_b3 = jnp.concatenate([now_b] * 3, axis=0)
    coarse = dot(table_a_ref[: 2 * half, :], hot_a3[:, : 2 * window])
    fine = dot(table_b_ref[...], now_b3)
    roots = dot(table_a_ref[2 * half :, :], hot_a3)
    cos_a, sin_a = coarse[:half], coarse[half:]
    cos_b, sin_b = fine[:half], fine[half:]
    feats = jnp.concatenate([cos_a * cos_b - sin_a * sin_b, sin_a * cos_b + cos_a * sin_b], axis=0)
    temb = jnp.dot(time_ref[...], feats, preferred_element_type=F32, precision=lax.Precision.HIGHEST)
    root = jnp.sum(roots[:RADIX] * hot_b, axis=0, keepdims=True)
    rest = jnp.sum(roots[RADIX:] * hot_b, axis=0, keepdims=True)
    two = 2 * window
    coef_one = root[:, two:] / root[:, :two]
    coef_two = rest[:, two:] - coef_one * rest[:, :two]

    out_w = jnp.concatenate([out_w_ref[...]] * group, axis=0)
    spread = lax.broadcasted_iota(jnp.int32, (lat, depth), 0) == lax.broadcasted_iota(jnp.int32, (lat, depth), 1) % lat
    in_w = dot(in_ref[...], spread.astype(F32).astype(BF16))
    through = dot(out_w, in_w.astype(BF16))
    in_half = (in_w * 0.5).astype(BF16)
    left_in[:channels, :depth] = in_half
    left_in[:channels, depth:] = jnp.zeros_like(in_half)
    high, low = split2(through)
    left_in[channels:, :depth] = high
    left_in[channels:, depth:] = low
    left_out[...] = out_w
    mid_half[...] = (mid_ref[...].astype(F32) * 0.5).astype(BF16)
    parts = split3(temb)
    bias_all = dot(out_w, parts[0]) + dot(out_w, parts[1]) + dot(out_w, parts[2])
    for r in range(ROUNDS):
        lanes = slice(r * window, (r + 1) * window)
        embed[r] = temb[:, lanes] * 0.5
        scale_x[r] = coef_one[:, lanes] - 1.0
        scale_e[r] = coef_two[:, lanes]
        bias[r] = bias_all[:, lanes] * coef_two[:, lanes]

    state[...] = recv_ref[...].T
    squares[...] = jnp.zeros_like(squares)

    earlier = lax.broadcasted_iota(jnp.int32, (window, window), 0)
    later = lax.broadcasted_iota(jnp.int32, (window, window), 1)
    lane_group = lax.broadcasted_iota(jnp.int32, (depth, window), 0) // lat

    def iteration(i, carry):
        r = i // ITERS
        shift = jnp.where(i % ITERS == ITERS - 1, adv_ref[r], 0)
        keep = (earlier < later).astype(F32).astype(BF16)
        moved = (earlier < jnp.minimum(later + shift, window - 1)).astype(F32).astype(BF16)
        sums = jnp.concatenate([keep, moved], axis=1)
        time = embed[r]
        error = jnp.zeros((depth, window), F32)
        for t in range(tiles):
            at = slice(t * depth, (t + 1) * depth)
            x = state[at, :]
            own = [jnp.where(lane_group == g, x, 0.0).astype(BF16) for g in range(group)]
            right = jnp.concatenate(own, axis=1)
            right = jnp.concatenate([right, right], axis=0)
            first = dot(left_in[...], right)
            pre = first[:channels] + jnp.concatenate([time] * group, axis=1)
            hidden = (pre * jnp.tanh(pre) + pre).astype(BF16)
            mixed = dot(mid_half[...], hidden)
            second = (mixed * jnp.tanh(mixed) + mixed).astype(BF16)
            noise = dot(left_out[...], second) + first[channels:]
            picked = noise[:, :window]
            for g in range(1, group):
                picked = jnp.where(lane_group == g, noise[:, g * window : (g + 1) * window], picked)
            drift = scale_x[r] * x + scale_e[r] * picked + bias[r]
            both = sum(dot(part, sums) for part in split3(drift))
            head = x[:, :1]
            change = both[:, :window] + head - x
            error = error + change * change
            state[at, :] = both[:, window:] + head
        squares[pl.ds(i, 1), :] = jnp.sum(error, axis=0, keepdims=True)
        return carry

    lax.fori_loop(0, iters, iteration, 0)
    send_ref[:, :rows] = state[...].T
    send_ref[:, rows:] = squares[...].T


def solve(advances, stamps, received, in_weight, time_weight, mid_weight, out_weight, group):
    window, rows = received.shape
    channels, lat = in_weight.shape
    table_a, table_b = tables(channels)
    depth = group * lat
    vmem = pl.BlockSpec(memory_space=pltpu.VMEM)
    return pl.pallas_call(
        functools.partial(picard, group),
        name="picard",
        out_shape=jax.ShapeDtypeStruct((window, rows + window), F32),
        in_specs=[pl.BlockSpec(memory_space=pltpu.SMEM)] + [vmem] * 8,
        out_specs=vmem,
        scratch_shapes=[
            pltpu.VMEM((rows, window), F32),
            pltpu.VMEM((ROUNDS, channels, window), F32),
            pltpu.VMEM((ROUNDS, depth, window), F32),
            pltpu.VMEM((ROUNDS, 1, window), F32),
            pltpu.VMEM((ROUNDS, 1, window), F32),
            pltpu.VMEM((channels, channels), BF16),
            pltpu.VMEM((channels + depth, 2 * depth), BF16),
            pltpu.VMEM((depth, channels), BF16),
            pltpu.VMEM((window, window), F32),
        ],
    )(advances, stamps, received, in_weight, time_weight, mid_weight, out_weight, jnp.asarray(table_a), jnp.asarray(table_b))


def shards(states, t_sched, advances, in_weight, time_weight, mid_weight, out_weight):
    _, lat, pixels = states.shape
    window = lax.axis_size("steps")
    own = pixels // window
    start = jnp.stack([jnp.int32(0), advances[0]])
    stamps = jnp.stack(
        [lax.dynamic_slice_in_dim(t_sched, start[r] + n, window) for r in range(ROUNDS) for n in range(2)]
    )
    out_going = states[0].reshape(lat, own, window).transpose(2, 1, 0).reshape(window, own * lat)
    received = lax.all_to_all(out_going, "steps", 0, 0, tiled=True)
    send = solve(advances, stamps, received, in_weight, time_weight, mid_weight, out_weight, 4)
    back = lax.all_to_all(send, "steps", 0, 0, tiled=True)
    final = back[:, : own * lat].reshape(window, own, lat).transpose(2, 1, 0).reshape(1, lat, pixels)
    totals = jnp.sum(back[:, own * lat : own * lat + ROUNDS * ITERS], axis=0) / (lat * pixels)
    return final, totals.reshape(ROUNDS, ITERS, 1)


def solution(mesh):
    both = ("groups", "steps")
    in_specs = (P(both, None, None), P("groups"), P("groups"), P(), P(), P(), P())
    out_specs = (P(both, None, None), P("groups", None, "steps"))
    return jax.shard_map(shards, mesh=mesh, in_specs=in_specs, out_specs=out_specs, check_vma=False)
```

```python
import functools
import math

import jax
import jax.numpy as jnp
import ml_dtypes
import numpy as np
from jax import lax
from jax.experimental import pallas as pl
from jax.experimental.pallas import tpu as pltpu
from jax.sharding import PartitionSpec as P

TSTEPS = 1000
ITERS = 4
ROUNDS = 2
RADIX = 32
GROUP = 4
LIMIT = 16 * 1024 * 1024
F32 = jnp.float32
BF16 = jnp.bfloat16


def three_parts(table):
    rest = np.asarray(table, np.float64)
    parts = []
    for _ in range(3):
        part = rest.astype(ml_dtypes.bfloat16)
        parts.append(part)
        rest = rest - part.astype(np.float64)
    return np.concatenate(parts, axis=1)


def tables(width):
    half = width // 2
    freqs = np.exp(-math.log(10000.0) * np.arange(half, dtype=np.float64) / half)
    digits = np.arange(RADIX, dtype=np.float64)
    coarse = freqs[:, None] * (digits * RADIX)[None]
    fine = freqs[:, None] * digits[None]
    levels = np.arange(RADIX * RADIX, dtype=np.float64)
    low, high = math.sqrt(0.00085), math.sqrt(0.012)
    betas = (low + (high - low) * levels / (TSTEPS - 1)) ** 2
    alphas = np.exp(np.cumsum(np.log1p(-betas)))
    root = np.sqrt(alphas).reshape(RADIX, RADIX).T
    rest = np.sqrt(1.0 - alphas).reshape(RADIX, RADIX).T
    table_a = np.concatenate([np.cos(coarse), np.sin(coarse), root, rest], axis=0)
    table_b = np.concatenate([np.cos(fine), np.sin(fine)], axis=0)
    return three_parts(table_a), three_parts(table_b)


def dot(left, right):
    return jnp.dot(left, right, preferred_element_type=F32)


def split2(value):
    high = value.astype(BF16)
    return high, (value - high.astype(F32)).astype(BF16)


def split3(value):
    high = value.astype(BF16)
    rest = value - high.astype(F32)
    mid = rest.astype(BF16)
    return high, mid, (rest - mid.astype(F32)).astype(BF16)


def one_hot(row, count):
    return (lax.broadcasted_iota(jnp.int32, (count, row.shape[1]), 0) == row).astype(F32)


def arrange(states_ref, going_ref):
    _, lat, pixels = states_ref.shape
    window = going_ref.shape[0]
    blocks = [states_ref[0, :, p * window : (p + 1) * window] for p in range(pixels // window)]
    going_ref[...] = jnp.concatenate(blocks, axis=0).T


def prepare(
    group,
    adv_ref,
    stamps_ref,
    in_ref,
    time_ref,
    mid_ref,
    out_w_ref,
    table_a_ref,
    table_b_ref,
    embed,
    bias,
    scales,
    limits,
    mid_half,
    left_in,
    left_out,
):
    window = stamps_ref.shape[1]
    channels, lat = in_ref.shape
    half = channels // 2
    depth = group * lat

    stamps = stamps_ref[...]
    row = jnp.concatenate([stamps[k : k + 1] for k in (0, 2, 1, 3)], axis=1)
    hot_a = one_hot(row // RADIX, RADIX).astype(BF16)
    hot_b = one_hot(row % RADIX, RADIX)
    hot_a3 = jnp.concatenate([hot_a] * 3, axis=0)
    now_b = hot_b[:, : ROUNDS * window].astype(BF16)
    now_b3 = jnp.concatenate([now_b] * 3, axis=0)
    coarse = dot(table_a_ref[: 2 * half, :], hot_a3[:, : ROUNDS * window])
    fine = dot(table_b_ref[...], now_b3)
    roots = dot(table_a_ref[2 * half :, :], hot_a3)
    cos_a, sin_a = coarse[:half], coarse[half:]
    cos_b, sin_b = fine[:half], fine[half:]
    feats = jnp.concatenate([cos_a * cos_b - sin_a * sin_b, sin_a * cos_b + cos_a * sin_b], axis=0)
    temb = jnp.dot(time_ref[...], feats, preferred_element_type=F32, precision=lax.Precision.HIGHEST)
    root = jnp.sum(roots[:RADIX] * hot_b, axis=0, keepdims=True)
    rest = jnp.sum(roots[RADIX:] * hot_b, axis=0, keepdims=True)
    now = ROUNDS * window
    coef_one = root[:, now:] / root[:, :now]
    coef_two = rest[:, now:] - coef_one * rest[:, :now]

    out_w = jnp.concatenate([out_w_ref[...]] * group, axis=0)
    spread = lax.broadcasted_iota(jnp.int32, (lat, depth), 0) == lax.broadcasted_iota(jnp.int32, (lat, depth), 1) % lat
    in_w = dot(in_ref[...], spread.astype(F32).astype(BF16))
    through = dot(out_w, in_w.astype(BF16))
    in_half = (in_w * 0.5).astype(BF16)
    left_in[:channels, :depth] = in_half
    left_in[:channels, depth:] = jnp.zeros_like(in_half)
    high, low = split2(through)
    left_in[channels:, :depth] = high
    left_in[channels:, depth:] = low
    left_out[...] = out_w
    mid_half[...] = (mid_ref[...].astype(F32) * 0.5).astype(BF16)
    parts = split3(temb)
    bias_all = dot(out_w, parts[0]) + dot(out_w, parts[1]) + dot(out_w, parts[2])
    place = lax.broadcasted_iota(jnp.int32, (1, window), 1)
    for r in range(ROUNDS):
        lanes = slice(r * window, (r + 1) * window)
        embed[r] = temb[:, lanes] * 0.5
        scales[r, 0:1] = coef_one[:, lanes] - 1.0
        scales[r, 1:2] = coef_two[:, lanes]
        bias[r] = bias_all[:, lanes] * coef_two[:, lanes]
        for k in range(ITERS):
            shift = adv_ref[r] if k == ITERS - 1 else 0
            limits[r * ITERS + k : r * ITERS + k + 1, :] = jnp.minimum(place + shift, window - 1)


def picard(
    group,
    recv_ref,
    embed,
    bias,
    scales,
    limits,
    mid_half,
    left_in,
    left_out,
    send_ref,
    state,
    squares,
    hidden,
    second,
    direct,
):
    window, rows = recv_ref.shape
    channels = mid_half.shape[0]
    depth = left_out.shape[0]
    lat = depth // group
    tiles = rows // depth
    iters = ROUNDS * ITERS

    state[...] = recv_ref[...].T
    squares[...] = jnp.zeros_like(squares)
    earlier = lax.broadcasted_iota(jnp.int32, (window, window), 0)
    later = lax.broadcasted_iota(jnp.int32, (window, window), 1)
    lane_group = lax.broadcasted_iota(jnp.int32, (depth, window), 0) // lat

    def enter(i, t):
        x = state[t * depth : (t + 1) * depth, :]
        own = [jnp.where(lane_group == g, x, 0.0).astype(BF16) for g in range(group)]
        right = jnp.concatenate(own, axis=1)
        right = jnp.concatenate([right, right], axis=0)
        first = dot(left_in[...], right)
        time = embed[jnp.minimum(i, iters - 1) // ITERS]
        pre = first[:channels] + jnp.concatenate([time] * group, axis=1)
        hidden[t % 2] = (pre * jnp.tanh(pre) + pre).astype(BF16)
        direct[t % 4] = first[channels:]

    def mix(t):
        mixed = dot(mid_half[...], hidden[t % 2])
        second[t % 2] = (mixed * jnp.tanh(mixed) + mixed).astype(BF16)

    def leave(i, t, sums):
        r = i // ITERS
        at = slice(t * depth, (t + 1) * depth)
        x = state[at, :]
        noise = dot(left_out[...], second[t % 2]) + direct[t % 4]
        picked = noise[:, :window]
        for g in range(1, group):
            picked = jnp.where(lane_group == g, noise[:, g * window : (g + 1) * window], picked)
        drift = scales[r, 0:1] * x + scales[r, 1:2] * picked + bias[r]
        both = sum(dot(part, sums) for part in split3(drift))
        head = x[:, :1]
        change = both[:, :window] + head - x
        state[at, :] = both[:, window:] + head
        return change * change

    def sweep(i, carry):
        keep = (earlier < later).astype(F32).astype(BF16)
        moved = (earlier < limits[pl.ds(i, 1), :]).astype(F32).astype(BF16)
        sums = jnp.concatenate([keep, moved], axis=1)
        error = jnp.zeros((depth, window), F32)
        for t in range(tiles):
            enter(i + (t + 2) // tiles, (t + 2) % tiles)
            mix((t + 1) % tiles)
            error = error + leave(i, t, sums)
        squares[pl.ds(i, 1), :] = jnp.sum(error, axis=0, keepdims=True)
        return carry

    enter(0, 0)
    mix(0)
    enter(0, 1)
    lax.fori_loop(0, iters, sweep, 0)
    send_ref[pl.ds(0, window, stride=2), :] = state[...].T
    send_ref[pl.ds(1, window, stride=2), :] = squares[...].T


def finish(back_ref, final_ref, errors_ref):
    _, lat, pixels = final_ref.shape
    window = back_ref.shape[0] // 2
    rows = back_ref[pl.ds(0, window, stride=2), :].T
    for p in range(pixels // window):
        final_ref[0, :, p * window : (p + 1) * window] = rows[p * lat : (p + 1) * lat, :]
    totals = jnp.sum(back_ref[pl.ds(1, window, stride=2), :], axis=0, keepdims=True) * (1.0 / (lat * pixels))
    for r in range(ROUNDS):
        errors_ref[r] = totals[:, r * ITERS : (r + 1) * ITERS]


VMEM = pl.BlockSpec(memory_space=pltpu.VMEM)


def call(kernel, name, shapes, specs, scratch=(), limit=LIMIT):
    many = isinstance(shapes, (list, tuple))
    return pl.pallas_call(
        kernel,
        name=name,
        out_shape=shapes,
        in_specs=specs,
        out_specs=[VMEM] * len(shapes) if many else VMEM,
        scratch_shapes=list(scratch),
        compiler_params=pltpu.CompilerParams(vmem_limit_bytes=limit),
    )


def shape(dims, kind=F32):
    return jax.ShapeDtypeStruct(dims, kind)


def prep(advances, stamps, in_weight, time_weight, mid_weight, out_weight, group):
    channels, lat = in_weight.shape
    window = stamps.shape[1]
    depth = group * lat
    table_a, table_b = tables(channels)
    shapes = [
        shape((ROUNDS, channels, window)),
        shape((ROUNDS, depth, window)),
        shape((ROUNDS, 2, window)),
        shape((ROUNDS * ITERS, window), jnp.int32),
        shape((channels, channels), BF16),
        shape((channels + depth, 2 * depth), BF16),
        shape((depth, channels), BF16),
    ]
    specs = [pl.BlockSpec(memory_space=pltpu.SMEM)] + [VMEM] * 7
    return call(functools.partial(prepare, group), "prepare", shapes, specs)(
        advances, stamps, in_weight, time_weight, mid_weight, out_weight, jnp.asarray(table_a), jnp.asarray(table_b)
    )


def solve(received, ready, group):
    window, rows = received.shape
    channels = ready[4].shape[0]
    depth = ready[6].shape[0]
    scratch = [
        pltpu.VMEM((rows, window), F32),
        pltpu.VMEM((window, window), F32),
        pltpu.VMEM((2, channels, group * window), BF16),
        pltpu.VMEM((2, channels, group * window), BF16),
        pltpu.VMEM((4, depth, group * window), F32),
    ]
    kernel = functools.partial(picard, group)
    return call(kernel, "picard", shape((2 * window, rows)), [VMEM] * 8, scratch)(received, *ready)


def shards(states, t_sched, advances, in_weight, time_weight, mid_weight, out_weight):
    _, lat, pixels = states.shape
    window = lax.axis_size("steps")
    rows = lat * pixels // window
    start = jnp.stack([jnp.int32(0), advances[0]])
    stamps = jnp.stack(
        [lax.dynamic_slice_in_dim(t_sched, start[r] + n, window) for r in range(ROUNDS) for n in range(2)]
    )
    going = call(arrange, "arrange", shape((window, rows)), [VMEM])(states)
    received = lax.all_to_all(going, "steps", 0, 0, tiled=True)
    ready = prep(advances, stamps, in_weight, time_weight, mid_weight, out_weight, GROUP)
    send = solve(received, ready, GROUP)
    back = lax.all_to_all(send, "steps", 0, 0, tiled=True)
    final, errors = call(finish, "finish", [shape(states.shape), shape((ROUNDS, 1, ITERS))], [VMEM])(back)
    return final, errors.transpose(0, 2, 1)


def solution(mesh):
    both = ("groups", "steps")
    in_specs = (P(both, None, None), P("groups"), P("groups"), P(), P(), P(), P())
    out_specs = (P(both, None, None), P("groups", None, "steps"))
    return jax.shard_map(shards, mesh=mesh, in_specs=in_specs, out_specs=out_specs, check_vma=False)
```

```python
import functools
import math

import jax
import jax.numpy as jnp
import ml_dtypes
import numpy as np
from jax import lax
from jax.experimental import pallas as pl
from jax.experimental.pallas import tpu as pltpu
from jax.sharding import PartitionSpec as P

TSTEPS = 1000
ITERS = 4
ROUNDS = 2
RADIX = 32
GROUP = 4
LIMIT = 16 * 1024 * 1024
F32 = jnp.float32
BF16 = jnp.bfloat16


def three_parts(table):
    rest = np.asarray(table, np.float64)
    parts = []
    for _ in range(3):
        part = rest.astype(ml_dtypes.bfloat16)
        parts.append(part)
        rest = rest - part.astype(np.float64)
    return np.concatenate(parts, axis=1)


def tables(width):
    half = width // 2
    freqs = np.exp(-math.log(10000.0) * np.arange(half, dtype=np.float64) / half)
    digits = np.arange(RADIX, dtype=np.float64)
    coarse = freqs[:, None] * (digits * RADIX)[None]
    fine = freqs[:, None] * digits[None]
    levels = np.arange(RADIX * RADIX, dtype=np.float64)
    low, high = math.sqrt(0.00085), math.sqrt(0.012)
    betas = (low + (high - low) * levels / (TSTEPS - 1)) ** 2
    alphas = np.exp(np.cumsum(np.log1p(-betas)))
    root = np.sqrt(alphas).reshape(RADIX, RADIX).T
    rest = np.sqrt(1.0 - alphas).reshape(RADIX, RADIX).T
    table_a = np.concatenate([np.cos(coarse), np.sin(coarse), root, rest], axis=0)
    table_b = np.concatenate([np.cos(fine), np.sin(fine)], axis=0)
    return three_parts(table_a), three_parts(table_b)


def dot(left, right):
    return jnp.dot(left, right, preferred_element_type=F32)


def split2(value):
    high = value.astype(BF16)
    return high, (value - high.astype(F32)).astype(BF16)


def split3(value):
    high = value.astype(BF16)
    rest = value - high.astype(F32)
    mid = rest.astype(BF16)
    return high, mid, (rest - mid.astype(F32)).astype(BF16)


def one_hot(row, count):
    return (lax.broadcasted_iota(jnp.int32, (count, row.shape[1]), 0) == row).astype(F32)


def arrange(states_ref, going_ref):
    _, lat, pixels = states_ref.shape
    window = going_ref.shape[0]
    blocks = [states_ref[0, :, p * window : (p + 1) * window] for p in range(pixels // window)]
    going_ref[...] = jnp.concatenate(blocks, axis=0).T


def prepare(
    group,
    adv_ref,
    stamps_ref,
    in_ref,
    time_ref,
    mid_ref,
    out_w_ref,
    table_a_ref,
    table_b_ref,
    embed,
    bias,
    scales,
    limits,
    mid_half,
    left_in,
    left_out,
):
    window = stamps_ref.shape[1]
    channels, lat = in_ref.shape
    half = channels // 2
    depth = group * lat

    stamps = stamps_ref[...]
    row = jnp.concatenate([stamps[k : k + 1] for k in (0, 2, 1, 3)], axis=1)
    hot_a = one_hot(row // RADIX, RADIX).astype(BF16)
    hot_b = one_hot(row % RADIX, RADIX)
    hot_a3 = jnp.concatenate([hot_a] * 3, axis=0)
    now_b = hot_b[:, : ROUNDS * window].astype(BF16)
    now_b3 = jnp.concatenate([now_b] * 3, axis=0)
    coarse = dot(table_a_ref[: 2 * half, :], hot_a3[:, : ROUNDS * window])
    fine = dot(table_b_ref[...], now_b3)
    roots = dot(table_a_ref[2 * half :, :], hot_a3)
    cos_a, sin_a = coarse[:half], coarse[half:]
    cos_b, sin_b = fine[:half], fine[half:]
    feats = jnp.concatenate([cos_a * cos_b - sin_a * sin_b, sin_a * cos_b + cos_a * sin_b], axis=0)
    temb = jnp.dot(time_ref[...], feats, preferred_element_type=F32, precision=lax.Precision.HIGHEST)
    root = jnp.sum(roots[:RADIX] * hot_b, axis=0, keepdims=True)
    rest = jnp.sum(roots[RADIX:] * hot_b, axis=0, keepdims=True)
    now = ROUNDS * window
    coef_one = root[:, now:] / root[:, :now]
    coef_two = rest[:, now:] - coef_one * rest[:, :now]

    out_w = jnp.concatenate([out_w_ref[...]] * group, axis=0)
    spread = lax.broadcasted_iota(jnp.int32, (lat, depth), 0) == lax.broadcasted_iota(jnp.int32, (lat, depth), 1) % lat
    in_w = dot(in_ref[...], spread.astype(F32).astype(BF16))
    through = dot(out_w, in_w.astype(BF16))
    in_half = (in_w * 0.5).astype(BF16)
    left_in[:channels, :depth] = in_half
    left_in[:channels, depth:] = jnp.zeros_like(in_half)
    high, low = split2(through)
    left_in[channels:, :depth] = high
    left_in[channels:, depth:] = low
    left_out[...] = out_w
    mid_half[...] = (mid_ref[...].astype(F32) * 0.5).astype(BF16)
    parts = split3(temb)
    bias_all = dot(out_w, parts[0]) + dot(out_w, parts[1]) + dot(out_w, parts[2])
    place = lax.broadcasted_iota(jnp.int32, (1, window), 1)
    for r in range(ROUNDS):
        lanes = slice(r * window, (r + 1) * window)
        embed[r] = temb[:, lanes] * 0.5
        scales[r, 0:1] = coef_one[:, lanes] - 1.0
        scales[r, 1:2] = coef_two[:, lanes]
        bias[r] = bias_all[:, lanes] * coef_two[:, lanes]
        for k in range(ITERS):
            shift = adv_ref[r] if k == ITERS - 1 else 0
            limits[r * ITERS + k : r * ITERS + k + 1, :] = jnp.minimum(place + shift, window - 1)


def picard(
    group,
    recv_ref,
    embed,
    bias,
    scales,
    limits,
    mid_half,
    left_in,
    left_out,
    send_ref,
    state,
    squares,
    hidden,
    second,
    direct,
    noise,
    open_error,
):
    window, rows = recv_ref.shape
    channels = mid_half.shape[0]
    depth = left_out.shape[0]
    lat = depth // group
    tiles = rows // depth
    iters = ROUNDS * ITERS

    state[...] = recv_ref[...].T
    squares[...] = jnp.zeros_like(squares)
    earlier = lax.broadcasted_iota(jnp.int32, (window, window), 0)
    later = lax.broadcasted_iota(jnp.int32, (window, window), 1)
    lane_group = lax.broadcasted_iota(jnp.int32, (depth, window), 0) // lat

    def enter(i, t):
        x = state[t * depth : (t + 1) * depth, :]
        own = [jnp.where(lane_group == g, x, 0.0).astype(BF16) for g in range(group)]
        right = jnp.concatenate(own, axis=1)
        right = jnp.concatenate([right, right], axis=0)
        first = dot(left_in[...], right)
        time = embed[jnp.minimum(i, iters - 1) // ITERS]
        pre = first[:channels] + jnp.concatenate([time] * group, axis=1)
        hidden[t % 2] = (pre * jnp.tanh(pre) + pre).astype(BF16)
        direct[t % 4] = first[channels:]

    def mix(t):
        mixed = dot(mid_half[...], hidden[t % 2])
        second[t % 2] = (mixed * jnp.tanh(mixed) + mixed).astype(BF16)

    def leave(t):
        noise[t % 2] = dot(left_out[...], second[t % 2]) + direct[t % 4]

    def advance(i, t, sums, live):
        r = i // ITERS
        at = slice(t * depth, (t + 1) * depth)
        x = state[at, :]
        picked = noise[t % 2, :, :window]
        for g in range(1, group):
            picked = jnp.where(lane_group == g, noise[t % 2, :, g * window : (g + 1) * window], picked)
        drift = scales[r, 0:1] * x + scales[r, 1:2] * picked + bias[r]
        both = sum(dot(part, sums) for part in split3(drift))
        head = x[:, :1]
        change = both[:, :window] + head - x
        after = both[:, window:] + head
        state[at, :] = after if live is None else jnp.where(live, after, x)
        return change * change

    def sums_of(i):
        keep = (earlier < later).astype(F32).astype(BF16)
        moved = (earlier < limits[pl.ds(i, 1), :]).astype(F32).astype(BF16)
        return jnp.concatenate([keep, moved], axis=1)

    def close(i, error):
        squares[pl.ds(i, 1), :] = jnp.sum(error, axis=0, keepdims=True)

    def sweep(i, carry):
        error = jnp.zeros((depth, window), F32)
        for t in range(tiles):
            enter(i + (t + 2) // tiles, (t + 2) % tiles)
            mix((t + 1) % tiles)
            if t == 0:
                old = jnp.maximum(i - 1, 0)
                close(old, open_error[...] + advance(old, tiles - 1, sums_of(old), i > 0))
                sums = sums_of(i)
            else:
                error = error + advance(i, t - 1, sums, None)
            leave(t)
        open_error[...] = error
        return carry

    enter(0, 0)
    mix(0)
    enter(0, 1)
    lax.fori_loop(0, iters, sweep, 0)
    last = iters - 1
    close(last, open_error[...] + advance(last, tiles - 1, sums_of(last), None))
    send_ref[pl.ds(0, window, stride=2), :] = state[...].T
    send_ref[pl.ds(1, window, stride=2), :] = squares[...].T


def finish(back_ref, final_ref, errors_ref):
    _, lat, pixels = final_ref.shape
    window = back_ref.shape[0] // 2
    rows = back_ref[pl.ds(0, window, stride=2), :].T
    for p in range(pixels // window):
        final_ref[0, :, p * window : (p + 1) * window] = rows[p * lat : (p + 1) * lat, :]
    totals = jnp.sum(back_ref[pl.ds(1, window, stride=2), :], axis=0, keepdims=True) * (1.0 / (lat * pixels))
    for r in range(ROUNDS):
        errors_ref[r] = totals[:, r * ITERS : (r + 1) * ITERS]


VMEM = pl.BlockSpec(memory_space=pltpu.VMEM)


def call(kernel, name, shapes, specs, scratch=(), limit=LIMIT):
    many = isinstance(shapes, (list, tuple))
    return pl.pallas_call(
        kernel,
        name=name,
        out_shape=shapes,
        in_specs=specs,
        out_specs=[VMEM] * len(shapes) if many else VMEM,
        scratch_shapes=list(scratch),
        compiler_params=pltpu.CompilerParams(vmem_limit_bytes=limit),
    )


def shape(dims, kind=F32):
    return jax.ShapeDtypeStruct(dims, kind)


def prep(advances, stamps, in_weight, time_weight, mid_weight, out_weight, group):
    channels, lat = in_weight.shape
    window = stamps.shape[1]
    depth = group * lat
    table_a, table_b = tables(channels)
    shapes = [
        shape((ROUNDS, channels, window)),
        shape((ROUNDS, depth, window)),
        shape((ROUNDS, 2, window)),
        shape((ROUNDS * ITERS, window), jnp.int32),
        shape((channels, channels), BF16),
        shape((channels + depth, 2 * depth), BF16),
        shape((depth, channels), BF16),
    ]
    specs = [pl.BlockSpec(memory_space=pltpu.SMEM)] + [VMEM] * 7
    return call(functools.partial(prepare, group), "prepare", shapes, specs)(
        advances, stamps, in_weight, time_weight, mid_weight, out_weight, jnp.asarray(table_a), jnp.asarray(table_b)
    )


def solve(received, ready, group):
    window, rows = received.shape
    channels = ready[4].shape[0]
    depth = ready[6].shape[0]
    scratch = [
        pltpu.VMEM((rows, window), F32),
        pltpu.VMEM((window, window), F32),
        pltpu.VMEM((2, channels, group * window), BF16),
        pltpu.VMEM((2, channels, group * window), BF16),
        pltpu.VMEM((4, depth, group * window), F32),
        pltpu.VMEM((2, depth, group * window), F32),
        pltpu.VMEM((depth, window), F32),
    ]
    kernel = functools.partial(picard, group)
    return call(kernel, "picard", shape((2 * window, rows)), [VMEM] * 8, scratch)(received, *ready)


def shards(states, t_sched, advances, in_weight, time_weight, mid_weight, out_weight):
    _, lat, pixels = states.shape
    window = lax.axis_size("steps")
    rows = lat * pixels // window
    start = jnp.stack([jnp.int32(0), advances[0]])
    stamps = jnp.stack(
        [lax.dynamic_slice_in_dim(t_sched, start[r] + n, window) for r in range(ROUNDS) for n in range(2)]
    )
    going = call(arrange, "arrange", shape((window, rows)), [VMEM])(states)
    received = lax.all_to_all(going, "steps", 0, 0, tiled=True)
    ready = prep(advances, stamps, in_weight, time_weight, mid_weight, out_weight, GROUP)
    send = solve(received, ready, GROUP)
    back = lax.all_to_all(send, "steps", 0, 0, tiled=True)
    final, errors = call(finish, "finish", [shape(states.shape), shape((ROUNDS, 1, ITERS))], [VMEM])(back)
    return final, errors.transpose(0, 2, 1)


def solution(mesh):
    both = ("groups", "steps")
    in_specs = (P(both, None, None), P("groups"), P("groups"), P(), P(), P(), P())
    out_specs = (P(both, None, None), P("groups", None, "steps"))
    return jax.shard_map(shards, mesh=mesh, in_specs=in_specs, out_specs=out_specs, check_vma=False)
```

```python
import functools
import math

import jax
import jax.numpy as jnp
import ml_dtypes
import numpy as np
from jax import lax
from jax.experimental import pallas as pl
from jax.experimental.pallas import tpu as pltpu
from jax.sharding import Mesh
from jax.sharding import PartitionSpec as P

TSTEPS = 1000
ITERS = 4
ROUNDS = 2
RADIX = 32
GROUP = 4
LIMIT = 16 * 1024 * 1024
F32 = jnp.float32
BF16 = jnp.bfloat16


def three_parts(table):
    rest = np.asarray(table, np.float64)
    parts = []
    for _ in range(3):
        part = rest.astype(ml_dtypes.bfloat16)
        parts.append(part)
        rest = rest - part.astype(np.float64)
    return np.concatenate(parts, axis=1)


def tables(width):
    half = width // 2
    freqs = np.exp(-math.log(10000.0) * np.arange(half, dtype=np.float64) / half)
    digits = np.arange(RADIX, dtype=np.float64)
    coarse = freqs[:, None] * (digits * RADIX)[None]
    fine = freqs[:, None] * digits[None]
    levels = np.arange(RADIX * RADIX, dtype=np.float64)
    low, high = math.sqrt(0.00085), math.sqrt(0.012)
    betas = (low + (high - low) * levels / (TSTEPS - 1)) ** 2
    alphas = np.exp(np.cumsum(np.log1p(-betas)))
    root = np.sqrt(alphas).reshape(RADIX, RADIX).T
    rest = np.sqrt(1.0 - alphas).reshape(RADIX, RADIX).T
    table_a = np.concatenate([np.cos(coarse), np.sin(coarse), root, rest], axis=0)
    table_b = np.concatenate([np.cos(fine), np.sin(fine)], axis=0)
    return three_parts(table_a), three_parts(table_b)


def dot(left, right):
    return jnp.dot(left, right, preferred_element_type=F32)


def split2(value):
    high = value.astype(BF16)
    return high, (value - high.astype(F32)).astype(BF16)


def split3(value):
    high = value.astype(BF16)
    rest = value - high.astype(F32)
    mid = rest.astype(BF16)
    return high, mid, (rest - mid.astype(F32)).astype(BF16)


def one_hot(row, count):
    return (lax.broadcasted_iota(jnp.int32, (count, row.shape[1]), 0) == row).astype(F32)


def in_pairs(even, odd):
    own = lax.axis_index("cores") == 0
    return jnp.where(own, even, odd), jnp.where(own, odd, even)


def arrange(states_ref, keep_ref, give_ref, turned):
    _, lat, pixels = states_ref.shape
    window = turned.shape[0]
    blocks = [states_ref[0, :, p * window : (p + 1) * window] for p in range(pixels // window)]
    turned[...] = jnp.concatenate(blocks, axis=0).T
    half = pl.ds(0, window // 2, stride=2), pl.ds(1, window // 2, stride=2)
    keep_ref[...], give_ref[...] = in_pairs(turned[half[0], :], turned[half[1], :])


def merge(keep_ref, got_ref, both_ref):
    count = keep_ref.shape[0]
    both_ref[pl.ds(0, count, stride=2), :] = keep_ref[...]
    both_ref[pl.ds(1, count, stride=2), :] = got_ref[...]


def prepare(
    group,
    adv_ref,
    stamps_ref,
    in_ref,
    time_ref,
    mid_ref,
    out_w_ref,
    table_a_ref,
    table_b_ref,
    embed,
    bias,
    scales,
    limits,
    mid_half,
    left_in,
    left_out,
):
    window = stamps_ref.shape[1]
    channels, lat = in_ref.shape
    half = channels // 2
    depth = group * lat

    stamps = stamps_ref[...]
    row = jnp.concatenate([stamps[k : k + 1] for k in (0, 2, 1, 3)], axis=1)
    hot_a = one_hot(row // RADIX, RADIX).astype(BF16)
    hot_b = one_hot(row % RADIX, RADIX)
    hot_a3 = jnp.concatenate([hot_a] * 3, axis=0)
    now_b = hot_b[:, : ROUNDS * window].astype(BF16)
    now_b3 = jnp.concatenate([now_b] * 3, axis=0)
    coarse = dot(table_a_ref[: 2 * half, :], hot_a3[:, : ROUNDS * window])
    fine = dot(table_b_ref[...], now_b3)
    roots = dot(table_a_ref[2 * half :, :], hot_a3)
    cos_a, sin_a = coarse[:half], coarse[half:]
    cos_b, sin_b = fine[:half], fine[half:]
    feats = jnp.concatenate([cos_a * cos_b - sin_a * sin_b, sin_a * cos_b + cos_a * sin_b], axis=0)
    temb = jnp.dot(time_ref[...], feats, preferred_element_type=F32, precision=lax.Precision.HIGHEST)
    root = jnp.sum(roots[:RADIX] * hot_b, axis=0, keepdims=True)
    rest = jnp.sum(roots[RADIX:] * hot_b, axis=0, keepdims=True)
    now = ROUNDS * window
    coef_one = root[:, now:] / root[:, :now]
    coef_two = rest[:, now:] - coef_one * rest[:, :now]

    out_w = jnp.concatenate([out_w_ref[...]] * group, axis=0)
    spread = lax.broadcasted_iota(jnp.int32, (lat, depth), 0) == lax.broadcasted_iota(jnp.int32, (lat, depth), 1) % lat
    in_w = dot(in_ref[...], spread.astype(F32).astype(BF16))
    through = dot(out_w, in_w.astype(BF16))
    in_half = (in_w * 0.5).astype(BF16)
    left_in[:, :depth] = in_half
    left_in[:, depth:] = jnp.zeros_like(in_half)
    high, low = split2(through)
    left_out[:, :channels] = out_w
    left_out[:, channels : channels + depth] = high
    left_out[:, channels + depth :] = low
    mid_half[...] = (mid_ref[...].astype(F32) * 0.5).astype(BF16)
    parts = split3(temb)
    bias_all = dot(out_w, parts[0]) + dot(out_w, parts[1]) + dot(out_w, parts[2])
    place = lax.broadcasted_iota(jnp.int32, (1, window), 1)
    for r in range(ROUNDS):
        lanes = slice(r * window, (r + 1) * window)
        embed[r] = temb[:, lanes] * 0.5
        scales[r, 0:1] = coef_one[:, lanes] - 1.0
        scales[r, 1:2] = coef_two[:, lanes]
        bias[r] = bias_all[:, lanes] * coef_two[:, lanes]
        for k in range(ITERS):
            shift = adv_ref[r] if k == ITERS - 1 else 0
            limits[r * ITERS + k : r * ITERS + k + 1, :] = jnp.minimum(place + shift, window - 1)


def picard(
    group,
    recv_ref,
    embed,
    bias,
    scales,
    limits,
    mid_half,
    left_in,
    left_out,
    keep_ref,
    give_ref,
    state,
    squares,
    hidden,
    second,
    noise,
    open_error,
):
    window, rows = recv_ref.shape
    channels = mid_half.shape[0]
    depth = left_out.shape[0]
    lat = depth // group
    tiles = rows // depth
    iters = ROUNDS * ITERS

    half = pl.ds(0, window // 2, stride=2), pl.ds(1, window // 2, stride=2)
    squares[half[0], :], squares[half[1], :] = in_pairs(recv_ref[half[0], :], recv_ref[half[1], :])
    state[...] = squares[...].T
    squares[...] = jnp.zeros_like(squares)
    earlier = lax.broadcasted_iota(jnp.int32, (window, window), 0)
    later = lax.broadcasted_iota(jnp.int32, (window, window), 1)
    lane_group = lax.broadcasted_iota(jnp.int32, (depth, window), 0) // lat

    def enter(i, t):
        x = state[t * depth : (t + 1) * depth, :]
        own = [jnp.where(lane_group == g, x, 0.0).astype(BF16) for g in range(group)]
        right = jnp.concatenate(own, axis=1)
        right = jnp.concatenate([right, right], axis=0)
        first = dot(left_in[...], right)
        pre = first + jnp.concatenate([embed[i // ITERS]] * group, axis=1)
        hidden[t % 4, :channels] = (pre * jnp.tanh(pre) + pre).astype(BF16)
        second[t % 4, channels:] = right

    def mix(t):
        mixed = dot(mid_half[...], hidden[t % 4])
        second[t % 4, :channels] = (mixed * jnp.tanh(mixed) + mixed).astype(BF16)

    def leave(t):
        noise[t % 4] = dot(left_out[...], second[t % 4])

    def advance(i, t, sums, live):
        r = i // ITERS
        at = slice(t * depth, (t + 1) * depth)
        x = state[at, :]
        picked = noise[t % 4, :, :window]
        for g in range(1, group):
            picked = jnp.where(lane_group == g, noise[t % 4, :, g * window : (g + 1) * window], picked)
        drift = scales[r, 0:1] * x + scales[r, 1:2] * picked + bias[r]
        wide = dot(jnp.concatenate(split3(drift), axis=0), sums)
        both = wide[:depth] + wide[depth : 2 * depth] + wide[2 * depth :]
        head = x[:, :1]
        change = both[:, :window] + head - x
        after = both[:, window:] + head
        state[at, :] = after if live is None else jnp.where(live, after, x)
        return change * change

    def sums_of(i):
        keep = (earlier < later).astype(F32).astype(BF16)
        moved = (earlier < limits[pl.ds(i, 1), :]).astype(F32).astype(BF16)
        return jnp.concatenate([keep, moved], axis=1)

    def close(i, error):
        squares[pl.ds(i, 1), :] = jnp.sum(error, axis=0, keepdims=True)

    def sweep(i, carry, last=False):
        fixed = isinstance(i, int)
        old = max(i - 1, 0) if fixed else jnp.maximum(i - 1, 0)
        sums = sums_of(old)
        error = open_error[...]
        for t in range(tiles):
            if t == 2:
                close(old, error)
                sums = sums_of(i)
                error = jnp.zeros((depth, window), F32)
            if t < 2:
                error = error + advance(old, tiles + t - 2, sums, None if fixed else i > 0)
            else:
                error = error + advance(i, t - 2, sums, None)
            if not last or t + 2 < tiles:
                enter(i + (t + 2) // tiles, (t + 2) % tiles)
            if not last or t + 1 < tiles:
                mix((t + 1) % tiles)
            leave(t)
        open_error[...] = error
        return carry

    final = iters - 1
    for t in range(2):
        enter(0, t)
        if t < 1:
            mix(t)

    def several(j, carry):
        for u in range(3):
            sweep(j * 3 + u, carry)
        return carry

    whole = final // 3
    lax.fori_loop(0, whole, several, 0)
    for u in range(whole * 3, final):
        sweep(u, 0)
    sweep(final, 0, True)
    error = open_error[...]
    for t in range(tiles - 2, tiles):
        error = error + advance(final, t, sums_of(final), None)
    close(final, error)
    for kind, ref in enumerate((state, squares)):
        ref[...] = ref[...].T
        keep_ref[half[kind], :], give_ref[half[kind], :] = in_pairs(ref[half[0], :], ref[half[1], :])


def finish(back_ref, final_ref, errors_ref, rows):
    _, lat, pixels = final_ref.shape
    window = rows.shape[0]
    parts = [back_ref[pl.ds(k, window // 2, stride=4), :] for k in range(4)]
    rows[pl.ds(0, window // 2, stride=2), :], rows[pl.ds(1, window // 2, stride=2), :] = in_pairs(parts[0], parts[2])
    turned = rows[...].T
    for p in range(pixels // window):
        final_ref[0, :, p * window : (p + 1) * window] = turned[p * lat : (p + 1) * lat, :]
    totals = jnp.sum(parts[1] + parts[3], axis=0, keepdims=True) * (1.0 / (lat * pixels))
    for r in range(ROUNDS):
        errors_ref[r] = totals[:, r * ITERS : (r + 1) * ITERS]


VMEM = pl.BlockSpec(memory_space=pltpu.VMEM)


def call(kernel, name, shapes, specs, scratch=(), limit=LIMIT):
    many = isinstance(shapes, (list, tuple))
    return pl.pallas_call(
        kernel,
        name=name,
        out_shape=shapes,
        in_specs=specs,
        out_specs=[VMEM] * len(shapes) if many else VMEM,
        scratch_shapes=list(scratch),
        compiler_params=pltpu.CompilerParams(vmem_limit_bytes=limit),
    )


def shape(dims, kind=F32):
    return jax.ShapeDtypeStruct(dims, kind)


def prep(advances, stamps, in_weight, time_weight, mid_weight, out_weight, group):
    channels, lat = in_weight.shape
    window = stamps.shape[1]
    depth = group * lat
    table_a, table_b = tables(channels)
    shapes = [
        shape((ROUNDS, channels, window)),
        shape((ROUNDS, depth, window)),
        shape((ROUNDS, 2, window)),
        shape((ROUNDS * ITERS, window), jnp.int32),
        shape((channels, channels), BF16),
        shape((channels, 2 * depth), BF16),
        shape((depth, channels + 2 * depth), BF16),
    ]
    specs = [pl.BlockSpec(memory_space=pltpu.SMEM)] + [VMEM] * 7
    return call(functools.partial(prepare, group), "prepare", shapes, specs)(
        advances, stamps, in_weight, time_weight, mid_weight, out_weight, jnp.asarray(table_a), jnp.asarray(table_b)
    )


def solve(received, ready, group):
    window, rows = received.shape
    channels = ready[4].shape[0]
    depth = ready[6].shape[0]
    scratch = [
        pltpu.VMEM((rows, window), F32),
        pltpu.VMEM((window, window), F32),
        pltpu.VMEM((4, channels, group * window), BF16),
        pltpu.VMEM((4, channels + 2 * depth, group * window), BF16),
        pltpu.VMEM((4, depth, group * window), F32),
        pltpu.VMEM((depth, window), F32),
    ]
    kernel = functools.partial(picard, group)
    return call(kernel, "picard", [shape((window, rows))] * 2, [VMEM] * 8, scratch)(received, *ready)


def swap(give):
    return lax.ppermute(give, "cores", [(0, 1), (1, 0)])


def to_chips(rows):
    chips = lax.axis_size("chips")
    return lax.all_to_all(rows.reshape(chips, -1, rows.shape[-1]), "chips", 0, 0, tiled=True).reshape(-1, rows.shape[-1])


def shards(states, t_sched, advances, in_weight, time_weight, mid_weight, out_weight):
    _, lat, pixels = states.shape
    window = lax.axis_size(("chips", "cores"))
    rows = lat * pixels // window
    start = jnp.stack([jnp.int32(0), advances[0]])
    stamps = jnp.stack(
        [lax.dynamic_slice_in_dim(t_sched, start[r] + n, window) for r in range(ROUNDS) for n in range(2)]
    )
    halves = [shape((window // 2, rows))] * 2
    keep, give = call(arrange, "arrange", halves, [VMEM], [pltpu.VMEM((window, rows), F32)])(states)
    received = to_chips(call(merge, "merge", shape((window, rows)), [VMEM] * 2)(keep, swap(give)))
    ready = prep(advances, stamps, in_weight, time_weight, mid_weight, out_weight, GROUP)
    keep, give = solve(received, ready, GROUP)
    chips = lax.axis_size("chips")
    pair = [part.reshape(chips, -1, rows) for part in (keep, swap(give))]
    back = to_chips(jnp.concatenate(pair, axis=1).reshape(-1, rows))
    outs = [shape(states.shape), shape((ROUNDS, 1, ITERS))]
    final, errors = call(finish, "finish", outs, [VMEM], [pltpu.VMEM((window, rows), F32)])(back)
    return final, errors.transpose(0, 2, 1)


def solution(mesh):
    groups, steps = mesh.shape["groups"], mesh.shape["steps"]
    split = Mesh(mesh.devices.reshape(groups, steps // 2, 2), ("groups", "chips", "cores"))
    every = ("groups", "chips", "cores")
    in_specs = (P(every, None, None), P("groups"), P("groups"), P(), P(), P(), P())
    out_specs = (P(every, None, None), P("groups", None, every[1:]))
    return jax.shard_map(shards, mesh=split, in_specs=in_specs, out_specs=out_specs, check_vma=False)
```

```python
import functools
import math

import jax
import jax.numpy as jnp
import ml_dtypes
import numpy as np
from jax import lax
from jax.experimental import pallas as pl
from jax.experimental.pallas import tpu as pltpu
from jax.sharding import Mesh
from jax.sharding import PartitionSpec as P

TSTEPS = 1000
ITERS = 4
ROUNDS = 2
RADIX = 32
GROUP = 4
LANES = 128
LIMIT = 16 * 1024 * 1024
F32 = jnp.float32
BF16 = jnp.bfloat16


def three_parts(table):
    rest = np.asarray(table, np.float64)
    parts = []
    for _ in range(3):
        part = rest.astype(ml_dtypes.bfloat16)
        parts.append(part)
        rest = rest - part.astype(np.float64)
    return np.concatenate(parts, axis=1)


def tables(width):
    half = width // 2
    freqs = np.exp(-math.log(10000.0) * np.arange(half, dtype=np.float64) / half)
    digits = np.arange(RADIX, dtype=np.float64)
    coarse = freqs[:, None] * (digits * RADIX)[None]
    fine = freqs[:, None] * digits[None]
    levels = np.arange(RADIX * RADIX, dtype=np.float64)
    low, high = math.sqrt(0.00085), math.sqrt(0.012)
    betas = (low + (high - low) * levels / (TSTEPS - 1)) ** 2
    alphas = np.exp(np.cumsum(np.log1p(-betas)))
    root = np.sqrt(alphas).reshape(RADIX, RADIX).T
    rest = np.sqrt(1.0 - alphas).reshape(RADIX, RADIX).T
    table_a = np.concatenate([np.cos(coarse), np.sin(coarse), root, rest], axis=0)
    table_b = np.concatenate([np.cos(fine), np.sin(fine)], axis=0)
    return three_parts(table_a), three_parts(table_b)


def dot(left, right):
    return jnp.dot(left, right, preferred_element_type=F32)


def split2(value):
    high = value.astype(BF16)
    return high, (value - high.astype(F32)).astype(BF16)


def split3(value):
    high = value.astype(BF16)
    rest = value - high.astype(F32)
    mid = rest.astype(BF16)
    return high, mid, (rest - mid.astype(F32)).astype(BF16)


def one_hot(row, count):
    return (lax.broadcasted_iota(jnp.int32, (count, row.shape[1]), 0) == row).astype(F32)


def in_pairs(even, odd):
    own = lax.axis_index("cores") == 0
    return jnp.where(own, even, odd), jnp.where(own, odd, even)


def arrange(states_ref, keep_ref, give_ref, turned):
    _, lat, pixels = states_ref.shape
    window = turned.shape[0]
    blocks = [states_ref[0, :, p * window : (p + 1) * window] for p in range(pixels // window)]
    turned[...] = jnp.concatenate(blocks, axis=0).T
    half = pl.ds(0, window // 2, stride=2), pl.ds(1, window // 2, stride=2)
    keep_ref[...], give_ref[...] = in_pairs(turned[half[0], :], turned[half[1], :])


def merge(keep_ref, got_ref, both_ref):
    count = keep_ref.shape[0]
    both_ref[pl.ds(0, count, stride=2), :] = keep_ref[...]
    both_ref[pl.ds(1, count, stride=2), :] = got_ref[...]


def prepare(
    group,
    adv_ref,
    sched_ref,
    in_ref,
    time_ref,
    mid_ref,
    out_w_ref,
    table_a_ref,
    table_b_ref,
    embed,
    bias,
    scales,
    limits,
    mid_half,
    left_in,
    left_out,
    padded,
):
    window = embed.shape[2]
    channels, lat = in_ref.shape
    half = channels // 2
    depth = group * lat

    length = sched_ref.shape[1]
    padded[0:1, :length] = sched_ref[...]
    plan = padded[...]
    starts = [0, adv_ref[0]]
    rolled = [pltpu.roll(plan, padded.shape[1] - start - n, 1) if r or n else plan for n in range(2) for r, start in enumerate(starts)]
    row = jnp.concatenate([stamps[:1, :window] for stamps in rolled], axis=1)
    hot_a = one_hot(row // RADIX, RADIX).astype(BF16)
    hot_b = one_hot(row % RADIX, RADIX)
    hot_a3 = jnp.concatenate([hot_a] * 3, axis=0)
    now_b = hot_b[:, : ROUNDS * window].astype(BF16)
    now_b3 = jnp.concatenate([now_b] * 3, axis=0)
    coarse = dot(table_a_ref[: 2 * half, :], hot_a3[:, : ROUNDS * window])
    fine = dot(table_b_ref[...], now_b3)
    roots = dot(table_a_ref[2 * half :, :], hot_a3)
    cos_a, sin_a = coarse[:half], coarse[half:]
    cos_b, sin_b = fine[:half], fine[half:]
    feats = jnp.concatenate([cos_a * cos_b - sin_a * sin_b, sin_a * cos_b + cos_a * sin_b], axis=0)
    temb = jnp.dot(time_ref[...], feats, preferred_element_type=F32, precision=lax.Precision.HIGHEST)
    root = jnp.sum(roots[:RADIX] * hot_b, axis=0, keepdims=True)
    rest = jnp.sum(roots[RADIX:] * hot_b, axis=0, keepdims=True)
    now = ROUNDS * window
    coef_one = root[:, now:] / root[:, :now]
    coef_two = rest[:, now:] - coef_one * rest[:, :now]

    out_w = jnp.concatenate([out_w_ref[...]] * group, axis=0)
    spread = lax.broadcasted_iota(jnp.int32, (lat, depth), 0) == lax.broadcasted_iota(jnp.int32, (lat, depth), 1) % lat
    in_w = dot(in_ref[...], spread.astype(F32).astype(BF16))
    through = dot(out_w, in_w.astype(BF16))
    in_half = (in_w * 0.5).astype(BF16)
    left_in[:, :depth] = in_half
    left_in[:, depth:] = jnp.zeros_like(in_half)
    high, low = split2(through)
    left_out[:, :channels] = out_w
    left_out[:, channels : channels + depth] = high
    left_out[:, channels + depth :] = low
    mid_half[...] = (mid_ref[...].astype(F32) * 0.5).astype(BF16)
    parts = split3(temb)
    bias_all = dot(out_w, parts[0]) + dot(out_w, parts[1]) + dot(out_w, parts[2])
    place = lax.broadcasted_iota(jnp.int32, (1, window), 1)
    for r in range(ROUNDS):
        lanes = slice(r * window, (r + 1) * window)
        embed[r] = temb[:, lanes] * 0.5
        scales[r, 0:1] = coef_one[:, lanes] - 1.0
        scales[r, 1:2] = coef_two[:, lanes]
        bias[r] = bias_all[:, lanes] * coef_two[:, lanes]
        for k in range(ITERS):
            shift = adv_ref[r] if k == ITERS - 1 else 0
            limits[r * ITERS + k : r * ITERS + k + 1, :] = jnp.minimum(place + shift, window - 1)


def picard(
    group,
    recv_ref,
    embed,
    bias,
    scales,
    limits,
    mid_half,
    left_in,
    left_out,
    keep_ref,
    give_ref,
    state,
    squares,
    hidden,
    second,
    noise,
    open_error,
):
    window, rows = recv_ref.shape
    channels = mid_half.shape[0]
    depth = left_out.shape[0]
    lat = depth // group
    tiles = rows // depth
    iters = ROUNDS * ITERS

    half = pl.ds(0, window // 2, stride=2), pl.ds(1, window // 2, stride=2)
    squares[half[0], :], squares[half[1], :] = in_pairs(recv_ref[half[0], :], recv_ref[half[1], :])
    state[...] = squares[...].T
    squares[...] = jnp.zeros_like(squares)
    earlier = lax.broadcasted_iota(jnp.int32, (window, window), 0)
    later = lax.broadcasted_iota(jnp.int32, (window, window), 1)
    lane_group = lax.broadcasted_iota(jnp.int32, (depth, window), 0) // lat

    def enter(i, t):
        x = state[t * depth : (t + 1) * depth, :]
        own = [jnp.where(lane_group == g, x, 0.0).astype(BF16) for g in range(group)]
        right = jnp.concatenate(own, axis=1)
        right = jnp.concatenate([right, right], axis=0)
        first = dot(left_in[...], right)
        pre = first + jnp.concatenate([embed[i // ITERS]] * group, axis=1)
        hidden[t % 4, :channels] = (pre * jnp.tanh(pre) + pre).astype(BF16)
        second[t % 4, channels:] = right

    def mix(t):
        mixed = dot(mid_half[...], hidden[t % 4])
        second[t % 4, :channels] = (mixed * jnp.tanh(mixed) + mixed).astype(BF16)

    def leave(t):
        noise[t % 4] = dot(left_out[...], second[t % 4])

    def advance(i, t, sums, live):
        r = i // ITERS
        at = slice(t * depth, (t + 1) * depth)
        x = state[at, :]
        picked = noise[t % 4, :, :window]
        for g in range(1, group):
            picked = jnp.where(lane_group == g, noise[t % 4, :, g * window : (g + 1) * window], picked)
        drift = scales[r, 0:1] * x + scales[r, 1:2] * picked + bias[r]
        wide = dot(jnp.concatenate(split3(drift), axis=0), sums)
        both = wide[:depth] + wide[depth : 2 * depth] + wide[2 * depth :]
        head = x[:, :1]
        change = both[:, :window] + head - x
        after = both[:, window:] + head
        state[at, :] = after if live is None else jnp.where(live, after, x)
        return change * change

    def sums_of(i):
        keep = (earlier < later).astype(F32).astype(BF16)
        moved = (earlier < limits[pl.ds(i, 1), :]).astype(F32).astype(BF16)
        return jnp.concatenate([keep, moved], axis=1)

    def close(i, error):
        squares[pl.ds(i, 1), :] = jnp.sum(error, axis=0, keepdims=True)

    def sweep(i, carry, last=False):
        fixed = isinstance(i, int)
        old = max(i - 1, 0) if fixed else jnp.maximum(i - 1, 0)
        sums = sums_of(old)
        error = open_error[...]
        for t in range(tiles):
            if t == 2:
                close(old, error)
                sums = sums_of(i)
                error = jnp.zeros((depth, window), F32)
            if t < 2:
                error = error + advance(old, tiles + t - 2, sums, None if fixed else i > 0)
            else:
                error = error + advance(i, t - 2, sums, None)
            if not last or t + 2 < tiles:
                enter(i + (t + 2) // tiles, (t + 2) % tiles)
            if not last or t + 1 < tiles:
                mix((t + 1) % tiles)
            leave(t)
        open_error[...] = error
        return carry

    final = iters - 1
    for t in range(2):
        enter(0, t)
        if t < 1:
            mix(t)

    def several(j, carry):
        for u in range(3):
            sweep(j * 3 + u, carry)
        return carry

    whole = final // 3
    lax.fori_loop(0, whole, several, 0)
    for u in range(whole * 3, final):
        sweep(u, 0)
    sweep(final, 0, True)
    error = open_error[...]
    for t in range(tiles - 2, tiles):
        error = error + advance(final, t, sums_of(final), None)
    close(final, error)
    for kind, ref in enumerate((state, squares)):
        ref[...] = ref[...].T
        keep_ref[half[kind], :], give_ref[half[kind], :] = in_pairs(ref[half[0], :], ref[half[1], :])


def finish(back_ref, final_ref, errors_ref, rows):
    _, lat, pixels = final_ref.shape
    window = rows.shape[0]
    parts = [back_ref[pl.ds(k, window // 2, stride=4), :] for k in range(4)]
    rows[pl.ds(0, window // 2, stride=2), :], rows[pl.ds(1, window // 2, stride=2), :] = in_pairs(parts[0], parts[2])
    turned = rows[...].T
    for p in range(pixels // window):
        final_ref[0, :, p * window : (p + 1) * window] = turned[p * lat : (p + 1) * lat, :]
    totals = jnp.sum(parts[1] + parts[3], axis=0, keepdims=True) * (1.0 / (lat * pixels))
    for r in range(ROUNDS):
        errors_ref[r] = totals[:, r * ITERS : (r + 1) * ITERS]


VMEM = pl.BlockSpec(memory_space=pltpu.VMEM)


def call(kernel, name, shapes, specs, scratch=(), limit=LIMIT):
    many = isinstance(shapes, (list, tuple))
    return pl.pallas_call(
        kernel,
        name=name,
        out_shape=shapes,
        in_specs=specs,
        out_specs=[VMEM] * len(shapes) if many else VMEM,
        scratch_shapes=list(scratch),
        compiler_params=pltpu.CompilerParams(vmem_limit_bytes=limit),
    )


def shape(dims, kind=F32):
    return jax.ShapeDtypeStruct(dims, kind)


def prep(advances, t_sched, in_weight, time_weight, mid_weight, out_weight, group, window):
    channels, lat = in_weight.shape
    lanes = -(-t_sched.shape[0] // LANES) * LANES
    depth = group * lat
    table_a, table_b = tables(channels)
    shapes = [
        shape((ROUNDS, channels, window)),
        shape((ROUNDS, depth, window)),
        shape((ROUNDS, 2, window)),
        shape((ROUNDS * ITERS, window), jnp.int32),
        shape((channels, channels), BF16),
        shape((channels, 2 * depth), BF16),
        shape((depth, channels + 2 * depth), BF16),
    ]
    specs = [pl.BlockSpec(memory_space=pltpu.SMEM)] + [VMEM] * 7
    return call(functools.partial(prepare, group), "prepare", shapes, specs, [pltpu.VMEM((8, lanes), jnp.int32)])(
        advances, t_sched.reshape(1, -1), in_weight, time_weight, mid_weight, out_weight, jnp.asarray(table_a), jnp.asarray(table_b)
    )


def solve(received, ready, group):
    window, rows = received.shape
    channels = ready[4].shape[0]
    depth = ready[6].shape[0]
    scratch = [
        pltpu.VMEM((rows, window), F32),
        pltpu.VMEM((window, window), F32),
        pltpu.VMEM((4, channels, group * window), BF16),
        pltpu.VMEM((4, channels + 2 * depth, group * window), BF16),
        pltpu.VMEM((4, depth, group * window), F32),
        pltpu.VMEM((depth, window), F32),
    ]
    kernel = functools.partial(picard, group)
    return call(kernel, "picard", [shape((window, rows))] * 2, [VMEM] * 8, scratch)(received, *ready)


def swap(give):
    return lax.ppermute(give, "cores", [(0, 1), (1, 0)])


def to_chips(rows):
    chips = lax.axis_size("chips")
    return lax.all_to_all(rows.reshape(chips, -1, rows.shape[-1]), "chips", 0, 0, tiled=True).reshape(-1, rows.shape[-1])


def shards(states, t_sched, advances, in_weight, time_weight, mid_weight, out_weight):
    _, lat, pixels = states.shape
    window = lax.axis_size(("chips", "cores"))
    rows = lat * pixels // window
    halves = [shape((window // 2, rows))] * 2
    keep, give = call(arrange, "arrange", halves, [VMEM], [pltpu.VMEM((window, rows), F32)])(states)
    received = to_chips(call(merge, "merge", shape((window, rows)), [VMEM] * 2)(keep, swap(give)))
    ready = prep(advances, t_sched, in_weight, time_weight, mid_weight, out_weight, GROUP, window)
    keep, give = solve(received, ready, GROUP)
    chips = lax.axis_size("chips")
    pair = [part.reshape(chips, -1, rows) for part in (keep, swap(give))]
    back = to_chips(jnp.concatenate(pair, axis=1).reshape(-1, rows))
    outs = [shape(states.shape), shape((ROUNDS, 1, ITERS))]
    final, errors = call(finish, "finish", outs, [VMEM], [pltpu.VMEM((window, rows), F32)])(back)
    return final, errors.transpose(0, 2, 1)


def solution(mesh):
    groups, steps = mesh.shape["groups"], mesh.shape["steps"]
    split = Mesh(mesh.devices.reshape(groups, steps // 2, 2), ("groups", "chips", "cores"))
    every = ("groups", "chips", "cores")
    in_specs = (P(every, None, None), P("groups"), P("groups"), P(), P(), P(), P())
    out_specs = (P(every, None, None), P("groups", None, every[1:]))
    return jax.shard_map(shards, mesh=split, in_specs=in_specs, out_specs=out_specs, check_vma=False)
```

```python
import functools
import math

import jax
import jax.numpy as jnp
import ml_dtypes
import numpy as np
from jax import lax
from jax.experimental import pallas as pl
from jax.experimental.pallas import tpu as pltpu
from jax.sharding import Mesh
from jax.sharding import PartitionSpec as P

TSTEPS = 1000
ITERS = 4
ROUNDS = 2
RADIX = 32
GROUP = 4
BY_HAND = 64
LANES = 128
LIMIT = 16 * 1024 * 1024
F32 = jnp.float32
BF16 = jnp.bfloat16


def three_parts(table):
    rest = np.asarray(table, np.float64)
    parts = []
    for _ in range(3):
        part = rest.astype(ml_dtypes.bfloat16)
        parts.append(part)
        rest = rest - part.astype(np.float64)
    return np.concatenate(parts, axis=1)


def tables(width):
    half = width // 2
    freqs = np.exp(-math.log(10000.0) * np.arange(half, dtype=np.float64) / half)
    digits = np.arange(RADIX, dtype=np.float64)
    coarse = freqs[:, None] * (digits * RADIX)[None]
    fine = freqs[:, None] * digits[None]
    levels = np.arange(RADIX * RADIX, dtype=np.float64)
    low, high = math.sqrt(0.00085), math.sqrt(0.012)
    betas = (low + (high - low) * levels / (TSTEPS - 1)) ** 2
    alphas = np.exp(np.cumsum(np.log1p(-betas)))
    root = np.sqrt(alphas).reshape(RADIX, RADIX).T
    rest = np.sqrt(1.0 - alphas).reshape(RADIX, RADIX).T
    table_a = np.concatenate([np.cos(coarse), np.sin(coarse), root, rest], axis=0)
    table_b = np.concatenate([np.cos(fine), np.sin(fine)], axis=0)
    return three_parts(table_a), three_parts(table_b)


def dot(left, right):
    return jnp.dot(left, right, preferred_element_type=F32)


def split2(value):
    high = value.astype(BF16)
    return high, (value - high.astype(F32)).astype(BF16)


def split3(value):
    high = value.astype(BF16)
    rest = value - high.astype(F32)
    mid = rest.astype(BF16)
    return high, mid, (rest - mid.astype(F32)).astype(BF16)


def one_hot(row, count):
    return (lax.broadcasted_iota(jnp.int32, (count, row.shape[1]), 0) == row).astype(F32)


def in_pairs(even, odd):
    own = lax.axis_index("cores") == 0
    return jnp.where(own, even, odd), jnp.where(own, odd, even)


def arrange(states_ref, keep_ref, give_ref, turned):
    _, lat, pixels = states_ref.shape
    window = turned.shape[0]
    blocks = [states_ref[0, :, p * window : (p + 1) * window] for p in range(pixels // window)]
    turned[...] = jnp.concatenate(blocks, axis=0).T
    half = pl.ds(0, window // 2, stride=2), pl.ds(1, window // 2, stride=2)
    keep_ref[...], give_ref[...] = in_pairs(turned[half[0], :], turned[half[1], :])


def merge(keep_ref, got_ref, both_ref):
    count = keep_ref.shape[0]
    both_ref[pl.ds(0, count, stride=2), :] = keep_ref[...]
    both_ref[pl.ds(1, count, stride=2), :] = got_ref[...]


def cut(blocks, whole):
    for b in range(blocks.shape[0]):
        width = min(LANES, whole.shape[1] - b * LANES)
        blocks[b, :, :width] = whole[:, b * LANES : b * LANES + width]


def joined(blocks, width):
    return jnp.concatenate([blocks[b, :, : min(LANES, width - b * LANES)] for b in range(blocks.shape[0])], axis=1)


def prepare(
    group,
    adv_ref,
    sched_ref,
    in_ref,
    time_ref,
    mid_ref,
    out_w_ref,
    table_a_ref,
    table_b_ref,
    embed,
    bias,
    scales,
    limits,
    mid_half,
    left_in,
    left_out,
    spread_in,
    padded,
):
    window = embed.shape[2]
    channels, lat = in_ref.shape
    half = channels // 2
    depth = group * lat

    length = sched_ref.shape[1]
    padded[0:1, :length] = sched_ref[...]
    plan = padded[...]
    starts = [0, adv_ref[0]]
    rolled = [pltpu.roll(plan, padded.shape[1] - start - n, 1) if r or n else plan for n in range(2) for r, start in enumerate(starts)]
    row = jnp.concatenate([stamps[:1, :window] for stamps in rolled], axis=1)
    hot_a = one_hot(row // RADIX, RADIX).astype(BF16)
    hot_b = one_hot(row % RADIX, RADIX)
    hot_a3 = jnp.concatenate([hot_a] * 3, axis=0)
    now_b = hot_b[:, : ROUNDS * window].astype(BF16)
    now_b3 = jnp.concatenate([now_b] * 3, axis=0)
    coarse = dot(table_a_ref[: 2 * half, :], hot_a3[:, : ROUNDS * window])
    fine = dot(table_b_ref[...], now_b3)
    roots = dot(table_a_ref[2 * half :, :], hot_a3)
    cos_a, sin_a = coarse[:half], coarse[half:]
    cos_b, sin_b = fine[:half], fine[half:]
    feats = jnp.concatenate([cos_a * cos_b - sin_a * sin_b, sin_a * cos_b + cos_a * sin_b], axis=0)
    temb = jnp.dot(time_ref[...], feats, preferred_element_type=F32, precision=lax.Precision.HIGHEST)
    root = jnp.sum(roots[:RADIX] * hot_b, axis=0, keepdims=True)
    rest = jnp.sum(roots[RADIX:] * hot_b, axis=0, keepdims=True)
    now = ROUNDS * window
    coef_one = root[:, now:] / root[:, :now]
    coef_two = rest[:, now:] - coef_one * rest[:, :now]

    out_w = jnp.concatenate([out_w_ref[...]] * group, axis=0)
    spread = lax.broadcasted_iota(jnp.int32, (lat, depth), 0) == lax.broadcasted_iota(jnp.int32, (lat, depth), 1) % lat
    in_w = dot(in_ref[...], spread.astype(F32).astype(BF16))
    through = dot(out_w, in_w.astype(BF16))
    in_half = (in_w * 0.5).astype(BF16)
    left_in[:, :depth] = in_half
    left_in[:, depth:] = jnp.zeros_like(in_half)
    high, low = split2(through)
    cut(left_out, jnp.concatenate([out_w, jnp.concatenate([high, low], axis=1)], axis=1))
    for c in range(lat):
        spread_in[c] = jnp.broadcast_to(in_half[channels - BY_HAND :, c : c + 1].astype(F32), (BY_HAND, window))
    cut(mid_half, (mid_ref[...].astype(F32) * 0.5).astype(BF16))
    parts = split3(temb)
    bias_all = dot(out_w, parts[0]) + dot(out_w, parts[1]) + dot(out_w, parts[2])
    place = lax.broadcasted_iota(jnp.int32, (1, window), 1)
    for r in range(ROUNDS):
        lanes = slice(r * window, (r + 1) * window)
        embed[r] = temb[:, lanes] * 0.5
        scales[r, 0:1] = coef_one[:, lanes] - 1.0
        scales[r, 1:2] = coef_two[:, lanes]
        bias[r] = bias_all[:, lanes] * coef_two[:, lanes]
        for k in range(ITERS):
            shift = adv_ref[r] if k == ITERS - 1 else 0
            limits[r * ITERS + k : r * ITERS + k + 1, :] = jnp.minimum(place + shift, window - 1)


def picard(
    group,
    recv_ref,
    embed,
    bias,
    scales,
    limits,
    mid_half,
    left_in,
    left_out,
    spread_in,
    keep_ref,
    give_ref,
    state,
    squares,
    hidden,
    second,
    noise,
    open_error,
):
    window, rows = recv_ref.shape
    channels = mid_half.shape[1]
    depth = left_out.shape[1]
    lat = depth // group
    tiles = rows // depth
    iters = ROUNDS * ITERS

    half = pl.ds(0, window // 2, stride=2), pl.ds(1, window // 2, stride=2)
    squares[half[0], :], squares[half[1], :] = in_pairs(recv_ref[half[0], :], recv_ref[half[1], :])
    state[...] = squares[...].T
    squares[...] = jnp.zeros_like(squares)
    earlier = lax.broadcasted_iota(jnp.int32, (window, window), 0)
    later = lax.broadcasted_iota(jnp.int32, (window, window), 1)
    lane_group = lax.broadcasted_iota(jnp.int32, (depth, window), 0) // lat

    def enter(i, t):
        x = state[t * depth : (t + 1) * depth, :]
        own = [jnp.where(lane_group == g, x, 0.0).astype(BF16) for g in range(group)]
        right = jnp.concatenate(own, axis=1)
        right = jnp.concatenate([right, right], axis=0)
        low = x.astype(BF16).astype(F32)
        split = channels - BY_HAND
        first = dot(left_in[:split], right)
        pre = first + jnp.concatenate([embed[i // ITERS, :split]] * group, axis=1)
        hidden[t % 4, :split] = (pre * jnp.tanh(pre) + pre).astype(BF16)
        for g in range(group):
            pre = embed[i // ITERS, split:]
            for c in range(lat):
                pre = pre + spread_in[c] * low[g * lat + c : g * lat + c + 1, :]
            hidden[t % 4, split:, g * window : (g + 1) * window] = (pre * jnp.tanh(pre) + pre).astype(BF16)
        second[t % 4, channels:] = right

    def mix(t):
        mixed = dot(joined(mid_half, channels), hidden[t % 4])
        second[t % 4, :channels] = (mixed * jnp.tanh(mixed) + mixed).astype(BF16)

    def leave(t):
        noise[t % 4] = dot(joined(left_out, channels + 2 * depth), second[t % 4])

    def advance(i, t, sums, live):
        r = i // ITERS
        at = slice(t * depth, (t + 1) * depth)
        x = state[at, :]
        picked = noise[t % 4, :, :window]
        for g in range(1, group):
            picked = jnp.where(lane_group == g, noise[t % 4, :, g * window : (g + 1) * window], picked)
        drift = scales[r, 0:1] * x + scales[r, 1:2] * picked + bias[r]
        wide = dot(jnp.concatenate(split3(drift), axis=0), sums)
        both = wide[:depth] + wide[depth : 2 * depth] + wide[2 * depth :]
        head = x[:, :1]
        change = both[:, :window] + head - x
        after = both[:, window:] + head
        state[at, :] = after if live is None else jnp.where(live, after, x)
        return change * change

    def sums_of(i):
        keep = (earlier < later).astype(F32).astype(BF16)
        moved = (earlier < limits[pl.ds(i, 1), :]).astype(F32).astype(BF16)
        return jnp.concatenate([keep, moved], axis=1)

    def close(i, error):
        squares[pl.ds(i, 1), :] = jnp.sum(error, axis=0, keepdims=True)

    def sweep(i, carry, last=False):
        fixed = isinstance(i, int)
        old = max(i - 1, 0) if fixed else jnp.maximum(i - 1, 0)
        sums = sums_of(old)
        error = open_error[...]
        for t in range(tiles):
            if t == 2:
                close(old, error)
                sums = sums_of(i)
                error = jnp.zeros((depth, window), F32)
            if t < 2:
                error = error + advance(old, tiles + t - 2, sums, None if fixed else i > 0)
            else:
                error = error + advance(i, t - 2, sums, None)
            if not last or t + 3 < tiles:
                enter(i + (t + 3) // tiles, (t + 3) % tiles)
            if not last or t + 1 < tiles:
                mix((t + 1) % tiles)
            leave(t)
        open_error[...] = error
        return carry

    final = iters - 1
    for t in range(3):
        enter(0, t)
        if t < 1:
            mix(t)

    def several(j, carry):
        for u in range(3):
            sweep(j * 3 + u, carry)
        return carry

    whole = final // 3
    lax.fori_loop(0, whole, several, 0)
    for u in range(whole * 3, final):
        sweep(u, 0)
    sweep(final, 0, True)
    error = open_error[...]
    for t in range(tiles - 2, tiles):
        error = error + advance(final, t, sums_of(final), None)
    close(final, error)
    for kind, ref in enumerate((state, squares)):
        ref[...] = ref[...].T
        keep_ref[half[kind], :], give_ref[half[kind], :] = in_pairs(ref[half[0], :], ref[half[1], :])


def finish(back_ref, final_ref, errors_ref, rows):
    _, lat, pixels = final_ref.shape
    window = rows.shape[0]
    parts = [back_ref[pl.ds(k, window // 2, stride=4), :] for k in range(4)]
    rows[pl.ds(0, window // 2, stride=2), :], rows[pl.ds(1, window // 2, stride=2), :] = in_pairs(parts[0], parts[2])
    turned = rows[...].T
    for p in range(pixels // window):
        final_ref[0, :, p * window : (p + 1) * window] = turned[p * lat : (p + 1) * lat, :]
    totals = jnp.sum(parts[1] + parts[3], axis=0, keepdims=True) * (1.0 / (lat * pixels))
    for r in range(ROUNDS):
        errors_ref[r] = totals[:, r * ITERS : (r + 1) * ITERS]


VMEM = pl.BlockSpec(memory_space=pltpu.VMEM)


def call(kernel, name, shapes, specs, scratch=(), limit=LIMIT):
    many = isinstance(shapes, (list, tuple))
    return pl.pallas_call(
        kernel,
        name=name,
        out_shape=shapes,
        in_specs=specs,
        out_specs=[VMEM] * len(shapes) if many else VMEM,
        scratch_shapes=list(scratch),
        compiler_params=pltpu.CompilerParams(vmem_limit_bytes=limit),
    )


def shape(dims, kind=F32):
    return jax.ShapeDtypeStruct(dims, kind)


def prep(advances, t_sched, in_weight, time_weight, mid_weight, out_weight, group, window):
    channels, lat = in_weight.shape
    lanes = -(-t_sched.shape[0] // LANES) * LANES
    depth = group * lat
    table_a, table_b = tables(channels)
    shapes = [
        shape((ROUNDS, channels, window)),
        shape((ROUNDS, depth, window)),
        shape((ROUNDS, 2, window)),
        shape((ROUNDS * ITERS, window), jnp.int32),
        shape((-(-channels // LANES), channels, LANES), BF16),
        shape((channels, 2 * depth), BF16),
        shape((-(-(channels + 2 * depth) // LANES), depth, LANES), BF16),
        shape((lat, BY_HAND, window)),
    ]
    specs = [pl.BlockSpec(memory_space=pltpu.SMEM)] + [VMEM] * 7
    return call(functools.partial(prepare, group), "prepare", shapes, specs, [pltpu.VMEM((8, lanes), jnp.int32)])(
        advances, t_sched.reshape(1, -1), in_weight, time_weight, mid_weight, out_weight, jnp.asarray(table_a), jnp.asarray(table_b)
    )


def solve(received, ready, group):
    window, rows = received.shape
    channels = ready[4].shape[1]
    depth = ready[6].shape[1]
    scratch = [
        pltpu.VMEM((rows, window), F32),
        pltpu.VMEM((window, window), F32),
        pltpu.VMEM((4, channels, group * window), BF16),
        pltpu.VMEM((4, channels + 2 * depth, group * window), BF16),
        pltpu.VMEM((4, depth, group * window), F32),
        pltpu.VMEM((depth, window), F32),
    ]
    kernel = functools.partial(picard, group)
    return call(kernel, "picard", [shape((window, rows))] * 2, [VMEM] * 9, scratch)(received, *ready)


def swap(give):
    return lax.ppermute(give, "cores", [(0, 1), (1, 0)])


def to_chips(rows):
    chips = lax.axis_size("chips")
    return lax.all_to_all(rows.reshape(chips, -1, rows.shape[-1]), "chips", 0, 0, tiled=True).reshape(-1, rows.shape[-1])


def shards(states, t_sched, advances, in_weight, time_weight, mid_weight, out_weight):
    _, lat, pixels = states.shape
    window = lax.axis_size(("chips", "cores"))
    rows = lat * pixels // window
    halves = [shape((window // 2, rows))] * 2
    keep, give = call(arrange, "arrange", halves, [VMEM], [pltpu.VMEM((window, rows), F32)])(states)
    received = to_chips(call(merge, "merge", shape((window, rows)), [VMEM] * 2)(keep, swap(give)))
    ready = prep(advances, t_sched, in_weight, time_weight, mid_weight, out_weight, GROUP, window)
    keep, give = solve(received, ready, GROUP)
    chips = lax.axis_size("chips")
    pair = [part.reshape(chips, -1, rows) for part in (keep, swap(give))]
    back = to_chips(jnp.concatenate(pair, axis=1).reshape(-1, rows))
    outs = [shape(states.shape), shape((ROUNDS, 1, ITERS))]
    final, errors = call(finish, "finish", outs, [VMEM], [pltpu.VMEM((window, rows), F32)])(back)
    return final, errors.transpose(0, 2, 1)


def solution(mesh):
    groups, steps = mesh.shape["groups"], mesh.shape["steps"]
    split = Mesh(mesh.devices.reshape(groups, steps // 2, 2), ("groups", "chips", "cores"))
    every = ("groups", "chips", "cores")
    in_specs = (P(every, None, None), P("groups"), P("groups"), P(), P(), P(), P())
    out_specs = (P(every, None, None), P("groups", None, every[1:]))
    return jax.shard_map(shards, mesh=split, in_specs=in_specs, out_specs=out_specs, check_vma=False)
```

```python
import functools
import math

import jax
import jax.numpy as jnp
import ml_dtypes
import numpy as np
from jax import lax
from jax.experimental import pallas as pl
from jax.experimental.pallas import tpu as pltpu
from jax.sharding import Mesh
from jax.sharding import PartitionSpec as P

TSTEPS = 1000
ITERS = 4
ROUNDS = 2
RADIX = 32
GROUP = 4
BY_HAND = 64
LANES = 128
LIMIT = 16 * 1024 * 1024
F32 = jnp.float32
BF16 = jnp.bfloat16


def three_parts(table):
    rest = np.asarray(table, np.float64)
    parts = []
    for _ in range(3):
        part = rest.astype(ml_dtypes.bfloat16)
        parts.append(part)
        rest = rest - part.astype(np.float64)
    return np.concatenate(parts, axis=1)


def tables(width):
    half = width // 2
    freqs = np.exp(-math.log(10000.0) * np.arange(half, dtype=np.float64) / half)
    digits = np.arange(RADIX, dtype=np.float64)
    coarse = freqs[:, None] * (digits * RADIX)[None]
    fine = freqs[:, None] * digits[None]
    levels = np.arange(RADIX * RADIX, dtype=np.float64)
    low, high = math.sqrt(0.00085), math.sqrt(0.012)
    betas = (low + (high - low) * levels / (TSTEPS - 1)) ** 2
    alphas = np.exp(np.cumsum(np.log1p(-betas)))
    root = np.sqrt(alphas).reshape(RADIX, RADIX).T
    rest = np.sqrt(1.0 - alphas).reshape(RADIX, RADIX).T
    table_a = np.concatenate([np.cos(coarse), np.sin(coarse), root, rest], axis=0)
    table_b = np.concatenate([np.cos(fine), np.sin(fine)], axis=0)
    return three_parts(table_a), three_parts(table_b)


def dot(left, right):
    return jnp.dot(left, right, preferred_element_type=F32)


def split2(value):
    high = value.astype(BF16)
    return high, (value - high.astype(F32)).astype(BF16)


def split3(value):
    high = value.astype(BF16)
    rest = value - high.astype(F32)
    mid = rest.astype(BF16)
    return high, mid, (rest - mid.astype(F32)).astype(BF16)


def one_hot(row, count):
    return (lax.broadcasted_iota(jnp.int32, (count, row.shape[1]), 0) == row).astype(F32)


def in_pairs(even, odd):
    own = lax.axis_index("cores") == 0
    return jnp.where(own, even, odd), jnp.where(own, odd, even)


def arrange(states_ref, keep_ref, give_ref, turned):
    _, lat, pixels = states_ref.shape
    window = turned.shape[0]
    blocks = [states_ref[0, :, p * window : (p + 1) * window] for p in range(pixels // window)]
    turned[...] = jnp.concatenate(blocks, axis=0).T
    half = pl.ds(0, window // 2, stride=2), pl.ds(1, window // 2, stride=2)
    keep_ref[...], give_ref[...] = in_pairs(turned[half[0], :], turned[half[1], :])


def merge(keep_ref, got_ref, both_ref):
    count = keep_ref.shape[0]
    both_ref[pl.ds(0, count, stride=2), :] = keep_ref[...]
    both_ref[pl.ds(1, count, stride=2), :] = got_ref[...]


def cut(blocks, whole):
    for b in range(blocks.shape[0]):
        width = min(LANES, whole.shape[1] - b * LANES)
        blocks[b, :, :width] = whole[:, b * LANES : b * LANES + width]


def joined(blocks, width):
    return jnp.concatenate([blocks[b, :, : min(LANES, width - b * LANES)] for b in range(blocks.shape[0])], axis=1)


def prepare(
    group,
    adv_ref,
    sched_ref,
    in_ref,
    time_ref,
    mid_ref,
    out_w_ref,
    table_a_ref,
    table_b_ref,
    embed,
    bias,
    scales,
    limits,
    mid_half,
    left_in,
    left_out,
    spread_in,
    padded,
):
    window = embed.shape[2]
    channels, lat = in_ref.shape
    half = channels // 2
    depth = group * lat

    length = sched_ref.shape[1]
    padded[0:1, :length] = sched_ref[...]
    plan = padded[...]
    starts = [0, adv_ref[0]]
    rolled = [pltpu.roll(plan, padded.shape[1] - start - n, 1) if r or n else plan for n in range(2) for r, start in enumerate(starts)]
    row = jnp.concatenate([stamps[:1, :window] for stamps in rolled], axis=1)
    hot_a = one_hot(row // RADIX, RADIX).astype(BF16)
    hot_b = one_hot(row % RADIX, RADIX)
    hot_a3 = jnp.concatenate([hot_a] * 3, axis=0)
    now_b = hot_b[:, : ROUNDS * window].astype(BF16)
    now_b3 = jnp.concatenate([now_b] * 3, axis=0)
    coarse = dot(table_a_ref[: 2 * half, :], hot_a3[:, : ROUNDS * window])
    fine = dot(table_b_ref[...], now_b3)
    roots = dot(table_a_ref[2 * half :, :], hot_a3)
    cos_a, sin_a = coarse[:half], coarse[half:]
    cos_b, sin_b = fine[:half], fine[half:]
    feats = jnp.concatenate([cos_a * cos_b - sin_a * sin_b, sin_a * cos_b + cos_a * sin_b], axis=0)
    temb = jnp.dot(time_ref[...], feats, preferred_element_type=F32, precision=lax.Precision.HIGHEST)
    root = jnp.sum(roots[:RADIX] * hot_b, axis=0, keepdims=True)
    rest = jnp.sum(roots[RADIX:] * hot_b, axis=0, keepdims=True)
    now = ROUNDS * window
    coef_one = root[:, now:] / root[:, :now]
    coef_two = rest[:, now:] - coef_one * rest[:, :now]

    out_w = jnp.concatenate([out_w_ref[...]] * group, axis=0)
    spread = lax.broadcasted_iota(jnp.int32, (lat, depth), 0) == lax.broadcasted_iota(jnp.int32, (lat, depth), 1) % lat
    in_w = dot(in_ref[...], spread.astype(F32).astype(BF16))
    through = dot(out_w, in_w.astype(BF16))
    in_half = (in_w * 0.5).astype(BF16)
    left_in[:, :depth] = in_half
    left_in[:, depth:] = jnp.zeros_like(in_half)
    high, low = split2(through)
    cut(left_out, jnp.concatenate([out_w, jnp.concatenate([high, low], axis=1)], axis=1))
    for c in range(lat):
        spread_in[c] = jnp.broadcast_to(in_half[channels - BY_HAND :, c : c + 1].astype(F32), (BY_HAND, window))
    cut(mid_half, (mid_ref[...].astype(F32) * 0.5).astype(BF16))
    parts = split3(temb)
    bias_all = dot(out_w, parts[0]) + dot(out_w, parts[1]) + dot(out_w, parts[2])
    place = lax.broadcasted_iota(jnp.int32, (1, window), 1)
    for r in range(ROUNDS):
        lanes = slice(r * window, (r + 1) * window)
        embed[r] = temb[:, lanes] * 0.5
        scales[r, 0:1] = coef_one[:, lanes] - 1.0
        scales[r, 1:2] = coef_two[:, lanes]
        bias[r] = bias_all[:, lanes] * coef_two[:, lanes]
        for k in range(ITERS):
            shift = adv_ref[r] if k == ITERS - 1 else 0
            limits[r * ITERS + k : r * ITERS + k + 1, :] = jnp.minimum(place + shift, window - 1)


def picard(
    group,
    recv_ref,
    embed,
    bias,
    scales,
    limits,
    mid_half,
    left_in,
    left_out,
    spread_in,
    keep_ref,
    give_ref,
    state,
    squares,
    hidden,
    second,
    noise,
    open_error,
):
    window, rows = recv_ref.shape
    channels = mid_half.shape[1]
    depth = left_out.shape[1]
    lat = depth // group
    tiles = rows // depth
    iters = ROUNDS * ITERS

    half = pl.ds(0, window // 2, stride=2), pl.ds(1, window // 2, stride=2)
    squares[half[0], :], squares[half[1], :] = in_pairs(recv_ref[half[0], :], recv_ref[half[1], :])
    state[...] = squares[...].T
    squares[...] = jnp.zeros_like(squares)
    earlier = lax.broadcasted_iota(jnp.int32, (window, window), 0)
    later = lax.broadcasted_iota(jnp.int32, (window, window), 1)
    lane_group = lax.broadcasted_iota(jnp.int32, (depth, window), 0) // lat

    def enter(i, t):
        x = state[t * depth : (t + 1) * depth, :]
        own = [jnp.where(lane_group == g, x, 0.0).astype(BF16) for g in range(group)]
        right = jnp.concatenate(own, axis=1)
        right = jnp.concatenate([right, right], axis=0)
        low = x.astype(BF16).astype(F32)
        split = channels - BY_HAND
        first = dot(left_in[:split], right)
        pre = first + jnp.concatenate([embed[i // ITERS, :split]] * group, axis=1)
        hidden[t % 4, :split] = (pre * jnp.tanh(pre) + pre).astype(BF16)
        for g in range(group):
            pre = embed[i // ITERS, split:]
            for c in range(lat):
                pre = pre + spread_in[c] * low[g * lat + c : g * lat + c + 1, :]
            hidden[t % 4, split:, g * window : (g + 1) * window] = (pre * jnp.tanh(pre) + pre).astype(BF16)
        second[t % 4, channels:] = right

    def mix(t):
        mixed = dot(joined(mid_half, channels), hidden[t % 4])
        second[t % 4, :channels] = (mixed * jnp.tanh(mixed) + mixed).astype(BF16)

    def leave(t):
        noise[t % 4] = dot(joined(left_out, channels + 2 * depth), second[t % 4])

    def advance(i, t, sums, live):
        r = i // ITERS
        at = slice(t * depth, (t + 1) * depth)
        x = state[at, :]
        picked = noise[t % 4, :, :window]
        for g in range(1, group):
            picked = jnp.where(lane_group == g, noise[t % 4, :, g * window : (g + 1) * window], picked)
        drift = scales[r, 0:1] * x + scales[r, 1:2] * picked + bias[r]
        wide = dot(jnp.concatenate(split2(drift), axis=0), sums)
        both = wide[:depth] + wide[depth:]
        head = x[:, :1]
        change = both[:, :window] + head - x
        after = both[:, window:] + head
        state[at, :] = after if live is None else jnp.where(live, after, x)
        return change * change

    def sums_of(i):
        keep = (earlier < later).astype(F32).astype(BF16)
        moved = (earlier < limits[pl.ds(i, 1), :]).astype(F32).astype(BF16)
        return jnp.concatenate([keep, moved], axis=1)

    def close(i, error):
        squares[pl.ds(i, 1), :] = jnp.sum(error, axis=0, keepdims=True)

    def sweep(i, carry, last=False):
        fixed = isinstance(i, int)
        old = max(i - 1, 0) if fixed else jnp.maximum(i - 1, 0)
        sums = sums_of(old)
        error = open_error[...]
        for t in range(tiles):
            if t == 2:
                close(old, error)
                sums = sums_of(i)
                error = jnp.zeros((depth, window), F32)
            if t < 2:
                error = error + advance(old, tiles + t - 2, sums, None if fixed else i > 0)
            else:
                error = error + advance(i, t - 2, sums, None)
            if not last or t + 3 < tiles:
                enter(i + (t + 3) // tiles, (t + 3) % tiles)
            if not last or t + 1 < tiles:
                mix((t + 1) % tiles)
            leave(t)
        open_error[...] = error
        return carry

    final = iters - 1
    for t in range(3):
        enter(0, t)
        if t < 1:
            mix(t)

    def several(j, carry):
        for u in range(3):
            sweep(j * 3 + u, carry)
        return carry

    whole = final // 3
    lax.fori_loop(0, whole, several, 0)
    for u in range(whole * 3, final):
        sweep(u, 0)
    sweep(final, 0, True)
    error = open_error[...]
    for t in range(tiles - 2, tiles):
        error = error + advance(final, t, sums_of(final), None)
    close(final, error)
    for kind, ref in enumerate((state, squares)):
        ref[...] = ref[...].T
        keep_ref[half[kind], :], give_ref[half[kind], :] = in_pairs(ref[half[0], :], ref[half[1], :])


def finish(back_ref, final_ref, errors_ref, rows):
    _, lat, pixels = final_ref.shape
    window = rows.shape[0]
    parts = [back_ref[pl.ds(k, window // 2, stride=4), :] for k in range(4)]
    rows[pl.ds(0, window // 2, stride=2), :], rows[pl.ds(1, window // 2, stride=2), :] = in_pairs(parts[0], parts[2])
    turned = rows[...].T
    for p in range(pixels // window):
        final_ref[0, :, p * window : (p + 1) * window] = turned[p * lat : (p + 1) * lat, :]
    totals = jnp.sum(parts[1] + parts[3], axis=0, keepdims=True) * (1.0 / (lat * pixels))
    for r in range(ROUNDS):
        errors_ref[r] = totals[:, r * ITERS : (r + 1) * ITERS]


VMEM = pl.BlockSpec(memory_space=pltpu.VMEM)


def call(kernel, name, shapes, specs, scratch=(), limit=LIMIT):
    many = isinstance(shapes, (list, tuple))
    return pl.pallas_call(
        kernel,
        name=name,
        out_shape=shapes,
        in_specs=specs,
        out_specs=[VMEM] * len(shapes) if many else VMEM,
        scratch_shapes=list(scratch),
        compiler_params=pltpu.CompilerParams(vmem_limit_bytes=limit),
    )


def shape(dims, kind=F32):
    return jax.ShapeDtypeStruct(dims, kind)


def prep(advances, t_sched, in_weight, time_weight, mid_weight, out_weight, group, window):
    channels, lat = in_weight.shape
    lanes = -(-t_sched.shape[0] // LANES) * LANES
    depth = group * lat
    table_a, table_b = tables(channels)
    shapes = [
        shape((ROUNDS, channels, window)),
        shape((ROUNDS, depth, window)),
        shape((ROUNDS, 2, window)),
        shape((ROUNDS * ITERS, window), jnp.int32),
        shape((-(-channels // LANES), channels, LANES), BF16),
        shape((channels, 2 * depth), BF16),
        shape((-(-(channels + 2 * depth) // LANES), depth, LANES), BF16),
        shape((lat, BY_HAND, window)),
    ]
    specs = [pl.BlockSpec(memory_space=pltpu.SMEM)] + [VMEM] * 7
    return call(functools.partial(prepare, group), "prepare", shapes, specs, [pltpu.VMEM((8, lanes), jnp.int32)])(
        advances, t_sched.reshape(1, -1), in_weight, time_weight, mid_weight, out_weight, jnp.asarray(table_a), jnp.asarray(table_b)
    )


def solve(received, ready, group):
    window, rows = received.shape
    channels = ready[4].shape[1]
    depth = ready[6].shape[1]
    scratch = [
        pltpu.VMEM((rows, window), F32),
        pltpu.VMEM((window, window), F32),
        pltpu.VMEM((4, channels, group * window), BF16),
        pltpu.VMEM((4, channels + 2 * depth, group * window), BF16),
        pltpu.VMEM((4, depth, group * window), F32),
        pltpu.VMEM((depth, window), F32),
    ]
    kernel = functools.partial(picard, group)
    return call(kernel, "picard", [shape((window, rows))] * 2, [VMEM] * 9, scratch)(received, *ready)


def swap(give):
    return lax.ppermute(give, "cores", [(0, 1), (1, 0)])


def to_chips(rows):
    chips = lax.axis_size("chips")
    return lax.all_to_all(rows.reshape(chips, -1, rows.shape[-1]), "chips", 0, 0, tiled=True).reshape(-1, rows.shape[-1])


def shards(states, t_sched, advances, in_weight, time_weight, mid_weight, out_weight):
    _, lat, pixels = states.shape
    window = lax.axis_size(("chips", "cores"))
    rows = lat * pixels // window
    halves = [shape((window // 2, rows))] * 2
    keep, give = call(arrange, "arrange", halves, [VMEM], [pltpu.VMEM((window, rows), F32)])(states)
    received = to_chips(call(merge, "merge", shape((window, rows)), [VMEM] * 2)(keep, swap(give)))
    ready = prep(advances, t_sched, in_weight, time_weight, mid_weight, out_weight, GROUP, window)
    keep, give = solve(received, ready, GROUP)
    chips = lax.axis_size("chips")
    pair = [part.reshape(chips, -1, rows) for part in (keep, swap(give))]
    back = to_chips(jnp.concatenate(pair, axis=1).reshape(-1, rows))
    outs = [shape(states.shape), shape((ROUNDS, 1, ITERS))]
    final, errors = call(finish, "finish", outs, [VMEM], [pltpu.VMEM((window, rows), F32)])(back)
    return final, errors.transpose(0, 2, 1)


def solution(mesh):
    groups, steps = mesh.shape["groups"], mesh.shape["steps"]
    split = Mesh(mesh.devices.reshape(groups, steps // 2, 2), ("groups", "chips", "cores"))
    every = ("groups", "chips", "cores")
    in_specs = (P(every, None, None), P("groups"), P("groups"), P(), P(), P(), P())
    out_specs = (P(every, None, None), P("groups", None, every[1:]))
    return jax.shard_map(shards, mesh=split, in_specs=in_specs, out_specs=out_specs, check_vma=False)
```
